8 devices in a mesh: tasks: 2 (over z, y), group: 4 (over x, core).
Axes of the slice: x: 2, y: 2, z: 1, core: 2. Of those that a mesh axis runs over, the one named last changes fastest.
Arguments:
- points: bfloat16 [16384, 384], P(('tasks', 'group')), parts along dimension 0
- vectors: bfloat16 [16384, 32], P(('tasks', 'group')), parts along dimension 0
- lengthscale: float32 [1], replicated
- outscale: float32 [1], replicated
Outputs:
- output: float32 [16384, 32], P(('tasks', 'group')), parts along dimension 0
There are 2 independent parts. The reference program is written for one: setup_inputs(seed, part) draws one part's arguments, and reference() takes and returns one part's arrays. A program takes and returns all parts, laid end to end along the dimension named above; an argument that names none is the same for every part.
All inputs are finite; a program needn't handle non-finite values.
Results may differ from the reference program's by a relative error of at most 0.001.
Values are sent between devices in bfloat16 or wider.
A program may use at most 1 GiB of HBM per device.

```python
import jax
import jax.numpy as jnp
from jax import lax

NUM_POINTS = 8192
FEAT_DIM = 384
NUM_RHS = 32
QUERY_BLOCK = 256
LATENT_DIM = 8


def setup_inputs(seed: int = 0, part: int = 0) -> dict:
    base_key = jax.random.key(seed)
    part_key = jax.random.fold_in(base_key, part)
    key_lat, key_mix, key_noise, key_rhs = jax.random.split(part_key, 4)
    key_ell, key_scale = jax.random.split(jax.random.key(seed + 29), 2)
    latent = jax.random.normal(key_lat, (NUM_POINTS, LATENT_DIM), jnp.float32)
    mixing = jax.random.normal(key_mix, (LATENT_DIM, FEAT_DIM), jnp.float32) * FEAT_DIM ** -0.5
    noise = jax.random.normal(key_noise, (NUM_POINTS, FEAT_DIM), jnp.float32) * (0.3 * FEAT_DIM ** -0.5)
    points = (jnp.dot(latent, mixing) + noise).astype(jnp.bfloat16)
    vectors = (jax.random.normal(key_rhs, (NUM_POINTS, NUM_RHS), jnp.float32) * NUM_POINTS ** -0.5).astype(jnp.bfloat16)
    lengthscale = jax.random.uniform(key_ell, (1,), jnp.float32, 2.4, 3.1)
    outscale = jax.random.uniform(key_scale, (1,), jnp.float32, 0.6, 1.6)
    return {'points': points, 'vectors': vectors, 'lengthscale': lengthscale, 'outscale': outscale}


def reference(points, vectors, lengthscale, outscale):
    sq_norm = jnp.sum(jnp.square(points.astype(jnp.float32)), axis=1)
    two_ell_sq = 2.0 * jnp.square(lengthscale[0])
    query_pts = points.reshape(NUM_POINTS // QUERY_BLOCK, QUERY_BLOCK, FEAT_DIM)
    query_norm = sq_norm.reshape(NUM_POINTS // QUERY_BLOCK, QUERY_BLOCK)

    def one_block(block_pair):
        block_pts, block_norm = block_pair
        gram_mat = jnp.dot(block_pts, points.T, preferred_element_type=jnp.float32)
        sq_dist = jnp.maximum(block_norm[:, None] + sq_norm[None, :] - 2.0 * gram_mat, 0.0)
        kern_blk = (outscale[0] * jnp.exp(-sq_dist / two_ell_sq)).astype(jnp.bfloat16)
        return jnp.dot(kern_blk, vectors, preferred_element_type=jnp.float32)

    result = lax.map(one_block, (query_pts, query_norm))
    return result.reshape(NUM_POINTS, NUM_RHS)
```

```python
import functools

import jax
import jax.numpy as jnp
from jax import lax
from jax.experimental import pallas as pl
from jax.experimental.pallas import tpu as pltpu
from jax.sharding import PartitionSpec as P

MESH = pl.DeviceIdType.MESH
F32 = jnp.float32
BF16 = jnp.bfloat16
LOG2E = 1.4426950408889634
ROWS, FEATS, RHS = 2048, 384, 32
STEP_R, STEP_C, SUB = 1024, 256, 256
CHUNKS = ROWS // STEP_C
DIRECT = (160, 160, 160, 176, 176, 176, 176, 176)
RELAY_MAX = STEP_C - min(DIRECT)
OWN, SIB, FAR = 0, ROWS, 2 * ROWS

NT = (((1,), (1,)), ((), ()))


def kernel(x_hbm, v_hbm, ell_ref, s_ref, out_ref,
           pts, vec, ncol, nrow, yloc, yfar, ysib, yret, relay, ka, kb,
           loc_sem, sib_send, sib_recv, dir_send, dir_recv, dirv_send, dirv_recv,
           hop_send, hop_recv, fwd_send, fwd_recv, ret_send, ret_recv):
    t = lax.axis_index('tasks')
    g = lax.axis_index('group')
    core = lax.rem(g, 2)
    heavy = lax.div(g, 2) == t
    light = jnp.logical_not(heavy)
    g_sib = g + 1 - 2 * core
    g_far = lax.rem(g + 2, 4)
    t_other = 1 - t

    load_x = pltpu.make_async_copy(x_hbm, pts.at[pl.ds(OWN, ROWS)], loc_sem.at[0])
    load_v = pltpu.make_async_copy(v_hbm, vec.at[:, pl.ds(OWN, ROWS)], loc_sem.at[1])
    load_x.start()
    load_v.start()
    barrier = pltpu.get_barrier_semaphore()
    for dev in ((t, g_sib), (t, g_far), (t_other, g), (t_other, g_far)):
        pl.semaphore_signal(barrier, inc=1, device_id=dev, device_id_type=MESH)

    def remote(src, dst, send, recv, dev):
        return pltpu.make_async_remote_copy(src_ref=src, dst_ref=dst, send_sem=send, recv_sem=recv,
                                            device_id=dev, device_id_type=MESH)

    def direct_x(k):
        lo, n = k * STEP_C, DIRECT[k]
        return remote(x_hbm.at[pl.ds(lo, n)], pts.at[pl.ds(FAR + lo, n)], dir_send.at[k], dir_recv.at[k], (t, g_far))

    def direct_v(k):
        lo = k * STEP_C
        return remote(v_hbm.at[:, pl.ds(lo, STEP_C)], vec.at[:, pl.ds(FAR + lo, STEP_C)],
                      dirv_send.at[k], dirv_recv.at[k], (t, g_far))

    def hop(k):
        lo, n = k * STEP_C + DIRECT[k], STEP_C - DIRECT[k]
        return remote(x_hbm.at[pl.ds(lo, n)], relay.at[k, pl.ds(0, n)], hop_send.at[k], hop_recv.at[k], (t_other, g))

    def forward(k):
        lo, n = k * STEP_C + DIRECT[k], STEP_C - DIRECT[k]
        return remote(relay.at[k, pl.ds(0, n)], pts.at[pl.ds(FAR + lo, n)], fwd_send.at[k], fwd_recv.at[k],
                      (t_other, g_far))

    def give_back(k):
        return remote(yfar.at[k], yret.at[k], ret_send.at[k], ret_recv.at[k], (t, g_far))

    sib_x = remote(x_hbm, pts.at[pl.ds(SIB, ROWS)], sib_send.at[0], sib_recv.at[0], (t, g_sib))
    sib_v = remote(v_hbm, vec.at[:, pl.ds(SIB, ROWS)], sib_send.at[1], sib_recv.at[1], (t, g_sib))
    sib_y = remote(yloc.at[:, pl.ds(SIB, ROWS)], ysib, sib_send.at[2], sib_recv.at[2], (t, g_sib))

    pl.semaphore_wait(barrier, 4)

    @pl.when(light)
    def _():
        for k in range(CHUNKS):
            direct_x(k).start()
            direct_v(k).start()
            hop(k).start()

    sib_x.start()
    sib_v.start()

    yloc[...] = jnp.zeros_like(yloc)
    yfar[...] = jnp.zeros_like(yfar)
    kb[...] = jnp.zeros_like(kb)
    ell = ell_ref[0]
    scale = s_ref[0]
    rate = -LOG2E / jnp.full((1, STEP_C), 2.0 * (ell * ell), F32)

    def norms(off, n, with_cols):
        for lo in range(0, n, 128):
            rows = pl.ds(pl.multiple_of(off + lo, 128), 128)
            x = pts[rows, :].astype(F32)
            block = jnp.broadcast_to(jnp.sum(x * x, axis=1, keepdims=True), (128, 128))
            if with_cols:
                ncol[rows, :] = block
            nrow[:, rows] = block.T[0:8, :]

    def all_norms(off):
        def some(i, _):
            norms(off + i * 256, 256, True)
            return 0
        lax.fori_loop(0, ROWS // 256, some, 0)

    def apply_k(k_buf, q, row, col, both):
        blk = k_buf[pl.ds(q * SUB, SUB), :]
        at = pl.ds(pl.multiple_of(row + q * SUB, SUB), SUB)
        yloc[:, at] += lax.dot_general(vec[:, pl.ds(col, STEP_C)], blk, NT, preferred_element_type=F32)
        if both:
            return jnp.dot(vec[:, at], blk, preferred_element_type=F32)
        return None

    def add_cols(col, acc, chunk):
        if chunk is None:
            yloc[:, pl.ds(col, STEP_C)] += acc
        else:
            yfar[chunk] += acc

    def step(slot, row, col, prev_row, prev_col, both, prev_chunk):
        new, old = (ka, kb) if slot == 0 else (kb, ka)
        acc = None
        for q in range(STEP_R // SUB):
            at = pl.ds(pl.multiple_of(row + q * SUB, SUB), SUB)
            gram = lax.dot_general(pts[at, :], pts[pl.ds(col, STEP_C), :], NT, preferred_element_type=F32)
            nc = ncol[at, :]
            dist = jnp.maximum((jnp.concatenate([nc, nc], axis=1) + nrow[0:1, pl.ds(col, STEP_C)]) - 2.0 * gram, 0.0)
            new[pl.ds(q * SUB, SUB), :] = (scale * jnp.exp2(dist * rate)).astype(BF16)
            part = apply_k(old, q, prev_row, prev_col, both)
            if both:
                acc = part if acc is None else acc + part
        if both:
            add_cols(prev_col, acc, prev_chunk)

    def drain(row, col, both, chunk):
        acc = None
        for q in range(STEP_R // SUB):
            part = apply_k(kb, q, row, col, both)
            if both:
                acc = part if acc is None else acc + part
        if both:
            add_cols(col, acc, chunk)

    def tile_rows(x):
        return pl.multiple_of(x, STEP_C)

    load_x.wait()
    load_v.wait()
    all_norms(OWN)

    def diag_body(i, _):
        base = i * STEP_R
        before = jnp.maximum(i - 1, 0) * STEP_R
        for q in range(4):
            if q == 0:
                prev = (tile_rows(before), tile_rows(before + 3 * STEP_C))
            else:
                prev = (tile_rows(base), tile_rows(base + (q - 1) * STEP_C))
            step(q % 2, tile_rows(base), tile_rows(base + q * STEP_C), *prev, False, None)
        return 0

    lax.fori_loop(0, 2, diag_body, 0)
    drain(STEP_R, STEP_R + 3 * STEP_C, False, None)
    kb[...] = jnp.zeros_like(kb)

    def pass_on(k):
        hop(k).wait_recv()
        forward(k).start()

    @pl.when(heavy)
    def _():
        pass_on(0)

    sib_x.wait_recv()
    sib_v.wait_recv()
    all_norms(SIB)

    def both_place(i):
        row = jnp.where(i == 0, STEP_R, core * (SIB + STEP_R))
        col = jnp.where(i == 0, 0, jnp.where(core == 0, SIB, OWN) + (i - 1) * STEP_R)
        return row, col

    def both_body(i, _):
        @pl.when(heavy)
        def _():
            for k in range(3):
                @pl.when(i == k)
                def _():
                    pass_on(k + 1)
        row, col = both_place(i)
        row0, col0 = both_place(jnp.maximum(i - 1, 0))
        for q in range(4):
            prev = (tile_rows(row0), tile_rows(col0 + 3 * STEP_C)) if q == 0 else (
                tile_rows(row), tile_rows(col + (q - 1) * STEP_C))
            step(q % 2, tile_rows(row), tile_rows(col + q * STEP_C), *prev, True, None)
        return 0

    lax.fori_loop(0, 3, both_body, 0)
    row_end, col_end = both_place(2)
    drain(tile_rows(row_end), tile_rows(col_end + 3 * STEP_C), True, None)

    @pl.when(heavy)
    def _():
        kb[...] = jnp.zeros_like(kb)
        order = (SIB, SIB + STEP_R, OWN, OWN + STEP_R)

        def far_body(k, _):
            for j in range(CHUNKS):
                @pl.when(k == j)
                def _():
                    if 1 <= j <= 4:
                        pass_on(j + 3)
                    direct_x(j).wait_recv()
                    direct_v(j).wait_recv()
                    forward(j).wait_recv()
            col = tile_rows(FAR + k * STEP_C)
            norms(col, STEP_C, False)
            before = jnp.maximum(k - 1, 0)
            for q in range(4):
                if q == 0:
                    step(0, order[0], col, order[3], tile_rows(FAR + before * STEP_C), True, before)
                else:
                    step(q % 2, order[q], col, order[q - 1], col, True, k)

            @pl.when(k > 0)
            def _():
                give_back(before).start()
            return 0

        lax.fori_loop(0, CHUNKS, far_body, 0)
        drain(order[3], FAR + (CHUNKS - 1) * STEP_C, True, CHUNKS - 1)
        give_back(CHUNKS - 1).start()

    sib_y.start()
    sib_y.wait_recv()

    @pl.when(heavy)
    def _():
        out_ref[...] = yloc[:, pl.ds(OWN, ROWS)] + ysib[...]
        for k in range(CHUNKS):
            forward(k).wait_send()
            give_back(k).wait_send()

    @pl.when(light)
    def _():
        for k in range(CHUNKS):
            at = pl.ds(k * STEP_C, STEP_C)
            give_back(k).wait_recv()
            out_ref[:, at] = yloc[:, at] + ysib[:, at] + yret[k]
            direct_x(k).wait_send()
            direct_v(k).wait_send()
            hop(k).wait_send()

    sib_x.wait_send()
    sib_v.wait_send()
    sib_y.wait_send()


def solution(mesh):
    row_spec = P(('tasks', 'group'), None)
    dma = pltpu.SemaphoreType.DMA

    def local_fn(x_loc, v_loc, lengthscale, outscale):
        any_spec = pl.BlockSpec(memory_space=pl.ANY)
        smem = pl.BlockSpec(memory_space=pltpu.SMEM)
        y_t = pl.pallas_call(
            kernel,
            out_shape=jax.ShapeDtypeStruct((RHS, ROWS), F32),
            in_specs=[any_spec, any_spec, smem, smem],
            out_specs=pl.BlockSpec(memory_space=pltpu.VMEM),
            scratch_shapes=[
                pltpu.VMEM((3 * ROWS, FEATS), BF16),
                pltpu.VMEM((RHS, 3 * ROWS), BF16),
                pltpu.VMEM((2 * ROWS, 128), F32),
                pltpu.VMEM((8, 3 * ROWS), F32),
                pltpu.VMEM((RHS, 2 * ROWS), F32),
                pltpu.VMEM((CHUNKS, RHS, STEP_C), F32),
                pltpu.VMEM((RHS, ROWS), F32),
                pltpu.VMEM((CHUNKS, RHS, STEP_C), F32),
                pltpu.VMEM((CHUNKS, RELAY_MAX, FEATS), BF16),
                pltpu.VMEM((STEP_R, STEP_C), BF16),
                pltpu.VMEM((STEP_R, STEP_C), BF16),
                dma((2,)), dma((3,)), dma((3,)),
            ] + [dma((CHUNKS,))] * 10,
            compiler_params=pltpu.CompilerParams(
                collective_id=0, has_side_effects=True, vmem_limit_bytes=60 * 2**20),
        )(x_loc, v_loc.T, lengthscale, outscale)
        return y_t.T

    return jax.shard_map(local_fn, mesh=mesh, in_specs=(row_spec, row_spec, P(None), P(None)), out_specs=row_spec,
                         check_vma=False)
```

```python
import functools

import jax
import jax.numpy as jnp
from jax import lax
from jax.experimental import pallas as pl
from jax.experimental.pallas import tpu as pltpu
from jax.sharding import PartitionSpec as P

MESH = pl.DeviceIdType.MESH
F32 = jnp.float32
BF16 = jnp.bfloat16
LOG2E = 1.4426950408889634
ROWS, FEATS, RHS = 2048, 384, 32
STEP_R, STEP_C, SUB = 1024, 256, 256
CHUNKS = ROWS // STEP_C
DIRECT = (160, 160, 160, 176, 176, 176, 176, 176)
RELAY_MAX = STEP_C - min(DIRECT)
OWN, SIB, FAR = 0, ROWS, 2 * ROWS
LENT = 2

NT = (((1,), (1,)), ((), ()))


def kernel(x_hbm, v_hbm, ell_ref, s_ref, out_ref,
           pts, vec, left, right, yloc, yfar, ysib, yret, relay, ka, kb,
           loc_sem, sib_send, sib_recv, dir_send, dir_recv, dirv_send, dirv_recv,
           hop_send, hop_recv, fwd_send, fwd_recv, ret_send, ret_recv):
    t = lax.axis_index('tasks')
    g = lax.axis_index('group')
    core = lax.rem(g, 2)
    heavy = lax.div(g, 2) == t
    light = jnp.logical_not(heavy)
    g_sib = g + 1 - 2 * core
    g_far = lax.rem(g + 2, 4)
    t_other = 1 - t

    load_x = pltpu.make_async_copy(x_hbm, pts.at[pl.ds(OWN, ROWS)], loc_sem.at[0])
    load_v = pltpu.make_async_copy(v_hbm, vec.at[:, pl.ds(OWN, ROWS)], loc_sem.at[1])
    load_x.start()
    load_v.start()
    barrier = pltpu.get_barrier_semaphore()
    for dev in ((t, g_sib), (t, g_far), (t_other, g), (t_other, g_far)):
        pl.semaphore_signal(barrier, inc=1, device_id=dev, device_id_type=MESH)

    def remote(src, dst, send, recv, dev):
        return pltpu.make_async_remote_copy(src_ref=src, dst_ref=dst, send_sem=send, recv_sem=recv,
                                            device_id=dev, device_id_type=MESH)

    def direct_x(k):
        lo, n = k * STEP_C, DIRECT[k]
        return remote(x_hbm.at[pl.ds(lo, n)], pts.at[pl.ds(FAR + lo, n)], dir_send.at[k], dir_recv.at[k], (t, g_far))

    def lent_x(k):
        at = pl.ds(k * STEP_C, STEP_C)
        return remote(x_hbm.at[at], pts.at[pl.ds(FAR + k * STEP_C, STEP_C)], dir_send.at[k], dir_recv.at[k], (t, g_far))

    def direct_v(k):
        lo = k * STEP_C
        return remote(v_hbm.at[:, pl.ds(lo, STEP_C)], vec.at[:, pl.ds(FAR + lo, STEP_C)],
                      dirv_send.at[k], dirv_recv.at[k], (t, g_far))

    def hop(k):
        lo, n = k * STEP_C + DIRECT[k], STEP_C - DIRECT[k]
        return remote(x_hbm.at[pl.ds(lo, n)], relay.at[k, pl.ds(0, n)], hop_send.at[k], hop_recv.at[k], (t_other, g))

    def forward(k):
        lo, n = k * STEP_C + DIRECT[k], STEP_C - DIRECT[k]
        return remote(relay.at[k, pl.ds(0, n)], pts.at[pl.ds(FAR + lo, n)], fwd_send.at[k], fwd_recv.at[k],
                      (t_other, g_far))

    def give_back(k):
        return remote(yfar.at[k], yret.at[k], ret_send.at[k], ret_recv.at[k], (t, g_far))

    sib_x = remote(x_hbm, pts.at[pl.ds(SIB, ROWS)], sib_send.at[0], sib_recv.at[0], (t, g_sib))
    sib_v = remote(v_hbm, vec.at[:, pl.ds(SIB, ROWS)], sib_send.at[1], sib_recv.at[1], (t, g_sib))
    sib_y = remote(yloc.at[:, pl.ds(SIB, ROWS)], ysib, sib_send.at[2], sib_recv.at[2], (t, g_sib))

    @pl.when(light)
    def _():
        pl.semaphore_wait(barrier, 4)
        for k in range(CHUNKS):
            direct_x(k).start()
            direct_v(k).start()
            hop(k).start()
        sib_x.start()
        sib_v.start()

    yloc[...] = jnp.zeros_like(yloc)
    yfar[...] = jnp.zeros_like(yfar)
    kb[...] = jnp.zeros_like(kb)
    ell = ell_ref[0]
    scale = s_ref[0]
    rate = -LOG2E / jnp.full((1, STEP_C), 2.0 * (ell * ell), F32)

    def split(n):
        high = n.astype(BF16).astype(F32)
        mid = (n - high).astype(BF16).astype(F32)
        return high, mid, (n - high) - mid

    def pick(index, parts):
        out = jnp.zeros_like(parts[0])
        for i, part in enumerate(parts):
            out = jnp.where(index == i, part, out)
        return out.astype(BF16)

    def norms(off, n, with_left):
        lane = lax.broadcasted_iota(jnp.int32, (128, 128), 1)
        one = jnp.ones((128, 128), F32)
        for lo in range(0, n, 128):
            rows = pl.ds(pl.multiple_of(off + lo, 128), 128)
            x = pts[rows, :].astype(F32)
            parts = split(jnp.broadcast_to(jnp.sum(x * x, axis=1, keepdims=True), (128, 128)))
            if with_left:
                left[rows, :] = pick(lane, (*parts, one, one, one))
            right[rows, :] = pick(lane, (one, one, one, *parts))

    def all_norms(off):
        def some(i, _):
            norms(off + i * 256, 256, True)
            return 0
        lax.fori_loop(0, ROWS // 256, some, 0)

    def apply_k(k_buf, q, row, col, both):
        blk = k_buf[pl.ds(q * SUB, SUB), :]
        at = pl.ds(pl.multiple_of(row + q * SUB, SUB), SUB)
        yloc[:, at] += lax.dot_general(vec[:, pl.ds(col, STEP_C)], blk, NT, preferred_element_type=F32)
        if both:
            return jnp.dot(vec[:, at], blk, preferred_element_type=F32)
        return None

    def add_cols(col, acc, chunk):
        if chunk is None:
            yloc[:, pl.ds(col, STEP_C)] += acc
        else:
            yfar[chunk] += acc

    def columns(col):
        at = pl.ds(col, STEP_C)
        return jnp.concatenate([pts[at, :] * BF16(-2.0), right[at, :]], axis=1)

    def step(slot, row, xr, prev_row, prev_col, both, prev_chunk):
        new, old = (ka, kb) if slot == 0 else (kb, ka)
        row, subs = row
        prev_row, prev_subs = prev_row
        acc = None
        for q in range(max(subs, prev_subs)):
            if q < subs:
                at = pl.ds(pl.multiple_of(row + q * SUB, SUB), SUB)
                xl = jnp.concatenate([pts[at, :], left[at, :]], axis=1)
                dist = jnp.maximum(lax.dot_general(xl, xr, NT, preferred_element_type=F32), 0.0)
                new[pl.ds(q * SUB, SUB), :] = (scale * jnp.exp2(dist * rate)).astype(BF16)
            if q < prev_subs:
                part = apply_k(old, q, prev_row, prev_col, both)
                if both:
                    acc = part if acc is None else acc + part
        if both:
            add_cols(prev_col, acc, prev_chunk)

    def drain(row, col, both, chunk):
        row, subs = row
        acc = None
        for q in range(subs):
            part = apply_k(kb, q, row, col, both)
            if both:
                acc = part if acc is None else acc + part
        if both:
            add_cols(col, acc, chunk)

    def tile_rows(x):
        return pl.multiple_of(x, STEP_C)

    load_x.wait()
    load_v.wait()
    all_norms(OWN)

    def diag_body(i, _):
        base = i * STEP_R
        before = jnp.maximum(i - 1, 0) * STEP_R
        for q in range(4):
            if q == 0:
                prev = ((tile_rows(before), 4), tile_rows(before + 3 * STEP_C))
            else:
                prev = ((tile_rows(base), 4), tile_rows(base + (q - 1) * STEP_C))
            step(q % 2, (tile_rows(base), 4), columns(tile_rows(base + q * STEP_C)), *prev, False, None)

        @pl.when(jnp.logical_and(heavy, i == 0))
        def _():
            pl.semaphore_wait(barrier, 4)
            sib_x.start()
            sib_v.start()
            for k in range(LENT):
                lent_x(k).start()
                direct_v(k).start()
        return 0

    lax.fori_loop(0, 2, diag_body, 0)
    drain((STEP_R, 4), STEP_R + 3 * STEP_C, False, None)
    kb[...] = jnp.zeros_like(kb)

    def pass_on(k):
        hop(k).wait_recv()
        forward(k).start()

    @pl.when(heavy)
    def _():
        pass_on(0)

    sib_x.wait_recv()
    sib_v.wait_recv()
    all_norms(SIB)

    def both_place(i):
        row = jnp.where(i == 0, STEP_R, core * (SIB + STEP_R))
        col = jnp.where(i == 0, 0, jnp.where(core == 0, SIB, OWN) + (i - 1) * STEP_R)
        return row, col

    def both_body(i, _):
        @pl.when(heavy)
        def _():
            for k in range(3):
                @pl.when(i == k)
                def _():
                    pass_on(k + 1)
        row, col = both_place(i)
        row0, col0 = both_place(jnp.maximum(i - 1, 0))
        for q in range(4):
            prev = ((tile_rows(row0), 4), tile_rows(col0 + 3 * STEP_C)) if q == 0 else (
                (tile_rows(row), 4), tile_rows(col + (q - 1) * STEP_C))
            step(q % 2, (tile_rows(row), 4), columns(tile_rows(col + q * STEP_C)), *prev, True, None)
        return 0

    lax.fori_loop(0, 3, both_body, 0)
    row_end, col_end = both_place(2)
    drain((tile_rows(row_end), 4), tile_rows(col_end + 3 * STEP_C), True, None)

    def far_pass(n, order, arrive):
        if n == 0:
            return
        kb[...] = jnp.zeros_like(kb)

        def far_body(k, _):
            for j in range(n):
                @pl.when(k == j)
                def _():
                    arrive(j)
            col = tile_rows(FAR + k * STEP_C)
            norms(col, STEP_C, False)
            xr = columns(col)
            before = jnp.maximum(k - 1, 0)
            for q in range(4):
                if q == 0:
                    step(0, order[0], xr, order[3], tile_rows(FAR + before * STEP_C), True, before)
                else:
                    step(q % 2, order[q], xr, order[q - 1], col, True, k)

            @pl.when(k > 0)
            def _():
                give_back(before).start()
            return 0

        lax.fori_loop(0, n, far_body, 0)
        drain(order[3], FAR + (n - 1) * STEP_C, True, n - 1)
        give_back(n - 1).start()

    def heavy_arrive(j):
        if j < 4:
            pass_on(j + 4)
        direct_x(j).wait_recv()
        direct_v(j).wait_recv()
        forward(j).wait_recv()

    def light_arrive(j):
        lent_x(j).wait_recv()
        direct_v(j).wait_recv()

    def near_rows(first):
        subs = (ROWS - first) // SUB
        more = (subs + 1) // 2
        return [piece for base in (SIB, OWN)
                for piece in ((base + first, more), (base + first + more * SUB, subs - more))]

    @pl.when(heavy)
    def _():
        far_pass(CHUNKS, near_rows(LENT * STEP_C), heavy_arrive)

    @pl.when(light)
    def _():
        far_pass(LENT, near_rows(0), light_arrive)

    sib_y.start()
    sib_y.wait_recv()

    @pl.when(heavy)
    def _():
        for k in range(CHUNKS):
            at = pl.ds(k * STEP_C, STEP_C)
            total = yloc[:, at] + ysib[:, at]
            if k < LENT:
                give_back(k).wait_recv()
                total = total + yret[k]
            out_ref[:, at] = total
            forward(k).wait_send()
            give_back(k).wait_send()
        for k in range(LENT):
            lent_x(k).wait_send()
            direct_v(k).wait_send()

    @pl.when(light)
    def _():
        for k in range(CHUNKS):
            at = pl.ds(k * STEP_C, STEP_C)
            give_back(k).wait_recv()
            out_ref[:, at] = yloc[:, at] + ysib[:, at] + yret[k]
            direct_x(k).wait_send()
            direct_v(k).wait_send()
            hop(k).wait_send()
        for k in range(LENT):
            give_back(k).wait_send()

    sib_x.wait_send()
    sib_v.wait_send()
    sib_y.wait_send()


def solution(mesh):
    row_spec = P(('tasks', 'group'), None)
    dma = pltpu.SemaphoreType.DMA

    def local_fn(x_loc, v_loc, lengthscale, outscale):
        any_spec = pl.BlockSpec(memory_space=pl.ANY)
        smem = pl.BlockSpec(memory_space=pltpu.SMEM)
        y_t = pl.pallas_call(
            kernel,
            out_shape=jax.ShapeDtypeStruct((RHS, ROWS), F32),
            in_specs=[any_spec, any_spec, smem, smem],
            out_specs=pl.BlockSpec(memory_space=pltpu.VMEM),
            scratch_shapes=[
                pltpu.VMEM((3 * ROWS, FEATS), BF16),
                pltpu.VMEM((RHS, 3 * ROWS), BF16),
                pltpu.VMEM((2 * ROWS, 128), BF16),
                pltpu.VMEM((3 * ROWS, 128), BF16),
                pltpu.VMEM((RHS, 2 * ROWS), F32),
                pltpu.VMEM((CHUNKS, RHS, STEP_C), F32),
                pltpu.VMEM((RHS, ROWS), F32),
                pltpu.VMEM((CHUNKS, RHS, STEP_C), F32),
                pltpu.VMEM((CHUNKS, RELAY_MAX, FEATS), BF16),
                pltpu.VMEM((STEP_R, STEP_C), BF16),
                pltpu.VMEM((STEP_R, STEP_C), BF16),
                dma((2,)), dma((3,)), dma((3,)),
            ] + [dma((CHUNKS,))] * 10,
            compiler_params=pltpu.CompilerParams(
                collective_id=0, has_side_effects=True, vmem_limit_bytes=60 * 2**20),
        )(x_loc, v_loc.T, lengthscale, outscale)
        return y_t.T

    return jax.shard_map(local_fn, mesh=mesh, in_specs=(row_spec, row_spec, P(None), P(None)), out_specs=row_spec,
                         check_vma=False)
```

```python
import functools

import jax
import jax.numpy as jnp
from jax import lax
from jax.experimental import pallas as pl
from jax.experimental.pallas import tpu as pltpu
from jax.sharding import PartitionSpec as P

MESH = pl.DeviceIdType.MESH
F32 = jnp.float32
BF16 = jnp.bfloat16
LOG2E = 1.4426950408889634
ROWS, FEATS, RHS = 2048, 384, 32
STEP_R, STEP_C, SUB = 1024, 256, 256
CHUNKS = ROWS // STEP_C
DIRECT = (176,) * 8
RELAY_MAX = STEP_C - min(DIRECT)
OWN, SIB, FAR = 0, ROWS, 2 * ROWS
LENT = 2

PASS_OWN = (0,)
PASS_BOTH = ((1,), (2,), (3,))
PASS_FAR = ((4,), (5,), (6,), (7,), (), (), (), ())

NT = (((1,), (1,)), ((), ()))


def kernel(x_hbm, v_hbm, ell_ref, s_ref, out_ref,
           pts, vec, left, right, yloc, yfar, ysib, yret, relay, ka, kb,
           loc_sem, go_sem, sib_send, sib_recv, dir_send, dir_recv, dirv_send, dirv_recv,
           hop_send, hop_recv, fwd_send, fwd_recv, ret_send, ret_recv):
    t = lax.axis_index('tasks')
    g = lax.axis_index('group')
    core = lax.rem(g, 2)
    heavy = lax.div(g, 2) == t
    light = jnp.logical_not(heavy)
    g_sib = g + 1 - 2 * core
    g_far = lax.rem(g + 2, 4)
    t_other = 1 - t

    load_x = pltpu.make_async_copy(x_hbm, pts.at[pl.ds(OWN, ROWS)], loc_sem.at[0])
    load_v = pltpu.make_async_copy(v_hbm, vec.at[:, pl.ds(OWN, ROWS)], loc_sem.at[1])
    load_x.start()
    load_v.start()
    barrier = pltpu.get_barrier_semaphore()
    far_sib = lax.rem(g_sib + 2, 4)

    def greet(*devices):
        for dev in devices:
            pl.semaphore_signal(barrier, inc=1, device_id=dev, device_id_type=MESH)

    @pl.when(heavy)
    def _():
        greet((t, g_far), (t_other, g), (t, g_sib), (t_other, g_far))

    @pl.when(light)
    def _():
        greet((t, g_far), (t_other, g), (t, far_sib))

    def remote(src, dst, send, recv, dev):
        return pltpu.make_async_remote_copy(src_ref=src, dst_ref=dst, send_sem=send, recv_sem=recv,
                                            device_id=dev, device_id_type=MESH)

    def direct_x(k):
        lo, n = k * STEP_C, DIRECT[k]
        return remote(x_hbm.at[pl.ds(lo, n)], pts.at[pl.ds(FAR + lo, n)], dir_send.at[k], dir_recv.at[k], (t, g_far))

    def lent_x(k):
        at = pl.ds(k * STEP_C, STEP_C)
        return remote(x_hbm.at[at], pts.at[pl.ds(FAR + k * STEP_C, STEP_C)], dir_send.at[k], dir_recv.at[k], (t, g_far))

    def direct_v(k):
        lo = k * STEP_C
        return remote(v_hbm.at[:, pl.ds(lo, STEP_C)], vec.at[:, pl.ds(FAR + lo, STEP_C)],
                      dirv_send.at[k], dirv_recv.at[k], (t, g_far))

    def hop(k):
        lo, n = k * STEP_C + DIRECT[k], STEP_C - DIRECT[k]
        return remote(x_hbm.at[pl.ds(lo, n)], relay.at[k, pl.ds(0, n)], hop_send.at[k], hop_recv.at[k], (t_other, g))

    def forward(k):
        lo, n = k * STEP_C + DIRECT[k], STEP_C - DIRECT[k]
        return remote(relay.at[k, pl.ds(0, n)], pts.at[pl.ds(FAR + lo, n)], fwd_send.at[k], fwd_recv.at[k],
                      (t_other, g_far))

    def give_back(k):
        return remote(yfar.at[k], yret.at[k], ret_send.at[k], ret_recv.at[k], (t, g_far))

    sib_x = remote(x_hbm, pts.at[pl.ds(SIB, ROWS)], sib_send.at[0], sib_recv.at[0], (t, g_sib))
    sib_v = remote(v_hbm, vec.at[:, pl.ds(SIB, ROWS)], sib_send.at[1], sib_recv.at[1], (t, g_sib))
    sib_y = remote(yloc.at[:, pl.ds(SIB, ROWS)], ysib, sib_send.at[2], sib_recv.at[2], (t, g_sib))

    @pl.when(light)
    def _():
        pl.semaphore_wait(barrier, 2)
        for k in range(CHUNKS):
            direct_x(k).start()
            direct_v(k).start()
            hop(k).start()

    yloc[...] = jnp.zeros_like(yloc)
    yfar[...] = jnp.zeros_like(yfar)
    kb[...] = jnp.zeros_like(kb)
    ell = ell_ref[0]
    scale = s_ref[0]
    rate = -LOG2E / jnp.full((1, STEP_C), 2.0 * (ell * ell), F32)

    def split(n):
        high = n.astype(BF16).astype(F32)
        mid = (n - high).astype(BF16).astype(F32)
        return high, mid, (n - high) - mid

    def pick(index, parts):
        out = jnp.zeros_like(parts[0])
        for i, part in enumerate(parts):
            out = jnp.where(index == i, part, out)
        return out.astype(BF16)

    def norms(off, n, with_left):
        lane = lax.broadcasted_iota(jnp.int32, (128, 128), 1)
        one = jnp.ones((128, 128), F32)
        for lo in range(0, n, 128):
            rows = pl.ds(pl.multiple_of(off + lo, 128), 128)
            x = pts[rows, :].astype(F32)
            parts = split(jnp.broadcast_to(jnp.sum(x * x, axis=1, keepdims=True), (128, 128)))
            if with_left:
                left[rows, :] = pick(lane, (*parts, one, one, one))
            right[rows, :] = pick(lane, (one, one, one, *parts))

    def all_norms(off):
        def some(i, _):
            norms(off + i * 256, 256, True)
            return 0
        lax.fori_loop(0, ROWS // 256, some, 0)

    def apply_k(k_buf, q, row, col, both):
        blk = k_buf[pl.ds(q * SUB, SUB), :]
        at = pl.ds(pl.multiple_of(row + q * SUB, SUB), SUB)
        yloc[:, at] += lax.dot_general(vec[:, pl.ds(col, STEP_C)], blk, NT, preferred_element_type=F32)
        if both:
            return jnp.dot(vec[:, at], blk, preferred_element_type=F32)
        return None

    def add_cols(col, acc, chunk):
        if chunk is None:
            yloc[:, pl.ds(col, STEP_C)] += acc
        else:
            yfar[chunk] += acc

    def columns(col):
        at = pl.ds(col, STEP_C)
        return jnp.concatenate([pts[at, :] * BF16(-2.0), right[at, :]], axis=1)

    def step(slot, row, xr, prev_row, prev_col, both, prev_chunk):
        new, old = (ka, kb) if slot == 0 else (kb, ka)
        row, subs = row
        prev_row, prev_subs = prev_row
        acc = None
        for q in range(max(subs, prev_subs)):
            if q < subs:
                at = pl.ds(pl.multiple_of(row + q * SUB, SUB), SUB)
                xl = jnp.concatenate([pts[at, :], left[at, :]], axis=1)
                dist = jnp.maximum(lax.dot_general(xl, xr, NT, preferred_element_type=F32), 0.0)
                new[pl.ds(q * SUB, SUB), :] = (scale * jnp.exp2(dist * rate)).astype(BF16)
            if q < prev_subs:
                part = apply_k(old, q, prev_row, prev_col, both)
                if both:
                    acc = part if acc is None else acc + part
        if both:
            add_cols(prev_col, acc, prev_chunk)

    def drain(row, col, both, chunk):
        row, subs = row
        acc = None
        for q in range(subs):
            part = apply_k(kb, q, row, col, both)
            if both:
                acc = part if acc is None else acc + part
        if both:
            add_cols(col, acc, chunk)

    def tile_rows(x):
        return pl.multiple_of(x, STEP_C)

    load_x.wait()
    load_v.wait()
    all_norms(OWN)

    def diag_body(i, _):
        base = i * STEP_R
        before = jnp.maximum(i - 1, 0) * STEP_R
        for q in range(4):
            if q == 0:
                prev = ((tile_rows(before), 4), tile_rows(before + 3 * STEP_C))
            else:
                prev = ((tile_rows(base), 4), tile_rows(base + (q - 1) * STEP_C))
            step(q % 2, (tile_rows(base), 4), columns(tile_rows(base + q * STEP_C)), *prev, False, None)

        @pl.when(jnp.logical_and(heavy, i == 0))
        def _():
            pl.semaphore_wait(barrier, 5)
            pl.semaphore_signal(go_sem, inc=1, device_id=(t, g_far), device_id_type=MESH)
            sib_x.start()
            sib_v.start()
            for k in range(LENT):
                lent_x(k).start()
                direct_v(k).start()

        @pl.when(jnp.logical_and(light, i == 1))
        def _():
            pl.semaphore_wait(go_sem, 1)
            sib_x.start()
            sib_v.start()
        return 0

    lax.fori_loop(0, 2, diag_body, 0)
    drain((STEP_R, 4), STEP_R + 3 * STEP_C, False, None)
    kb[...] = jnp.zeros_like(kb)

    def pass_on(k):
        hop(k).wait_recv()
        forward(k).start()

    @pl.when(heavy)
    def _():
        for k in PASS_OWN:
            pass_on(k)

    sib_x.wait_recv()
    sib_v.wait_recv()
    all_norms(SIB)

    def both_place(i):
        row = jnp.where(i == 0, STEP_R, core * (SIB + STEP_R))
        col = jnp.where(i == 0, 0, jnp.where(core == 0, SIB, OWN) + (i - 1) * STEP_R)
        return row, col

    def both_body(i, _):
        @pl.when(heavy)
        def _():
            for at, some in enumerate(PASS_BOTH):
                @pl.when(i == at)
                def _():
                    for k in some:
                        pass_on(k)
        row, col = both_place(i)
        row0, col0 = both_place(jnp.maximum(i - 1, 0))
        for q in range(4):
            prev = ((tile_rows(row0), 4), tile_rows(col0 + 3 * STEP_C)) if q == 0 else (
                (tile_rows(row), 4), tile_rows(col + (q - 1) * STEP_C))
            step(q % 2, (tile_rows(row), 4), columns(tile_rows(col + q * STEP_C)), *prev, True, None)
        return 0

    lax.fori_loop(0, 3, both_body, 0)
    row_end, col_end = both_place(2)
    drain((tile_rows(row_end), 4), tile_rows(col_end + 3 * STEP_C), True, None)

    def far_pass(n, order, arrive):
        if n == 0:
            return
        kb[...] = jnp.zeros_like(kb)

        def far_body(k, _):
            for j in range(n):
                @pl.when(k == j)
                def _():
                    arrive(j)
            col = tile_rows(FAR + k * STEP_C)
            norms(col, STEP_C, False)
            xr = columns(col)
            before = jnp.maximum(k - 1, 0)
            for q in range(4):
                if q == 0:
                    step(0, order[0], xr, order[3], tile_rows(FAR + before * STEP_C), True, before)
                else:
                    step(q % 2, order[q], xr, order[q - 1], col, True, k)

            @pl.when(k > 0)
            def _():
                give_back(before).start()
            return 0

        lax.fori_loop(0, n, far_body, 0)
        drain(order[3], FAR + (n - 1) * STEP_C, True, n - 1)
        give_back(n - 1).start()

    def heavy_arrive(j):
        for k in PASS_FAR[j]:
            pass_on(k)
        direct_x(j).wait_recv()
        direct_v(j).wait_recv()
        forward(j).wait_recv()

    def light_arrive(j):
        lent_x(j).wait_recv()
        direct_v(j).wait_recv()

    def near_rows(first):
        subs = (ROWS - first) // SUB
        more = (subs + 1) // 2
        return [piece for base in (SIB, OWN)
                for piece in ((base + first, more), (base + first + more * SUB, subs - more))]

    @pl.when(heavy)
    def _():
        far_pass(CHUNKS, near_rows(LENT * STEP_C), heavy_arrive)

    @pl.when(light)
    def _():
        far_pass(LENT, near_rows(0), light_arrive)

    sib_y.start()
    sib_y.wait_recv()

    @pl.when(heavy)
    def _():
        for k in range(CHUNKS):
            at = pl.ds(k * STEP_C, STEP_C)
            total = yloc[:, at] + ysib[:, at]
            if k < LENT:
                give_back(k).wait_recv()
                total = total + yret[k]
            out_ref[:, at] = total
            forward(k).wait_send()
            give_back(k).wait_send()
        for k in range(LENT):
            lent_x(k).wait_send()
            direct_v(k).wait_send()

    @pl.when(light)
    def _():
        for k in range(CHUNKS):
            at = pl.ds(k * STEP_C, STEP_C)
            give_back(k).wait_recv()
            out_ref[:, at] = yloc[:, at] + ysib[:, at] + yret[k]
            direct_x(k).wait_send()
            direct_v(k).wait_send()
            hop(k).wait_send()
        for k in range(LENT):
            give_back(k).wait_send()

    sib_x.wait_send()
    sib_v.wait_send()
    sib_y.wait_send()


def solution(mesh):
    row_spec = P(('tasks', 'group'), None)
    dma = pltpu.SemaphoreType.DMA

    def local_fn(x_loc, v_loc, lengthscale, outscale):
        any_spec = pl.BlockSpec(memory_space=pl.ANY)
        smem = pl.BlockSpec(memory_space=pltpu.SMEM)
        y_t = pl.pallas_call(
            kernel,
            out_shape=jax.ShapeDtypeStruct((RHS, ROWS), F32),
            in_specs=[any_spec, any_spec, smem, smem],
            out_specs=pl.BlockSpec(memory_space=pltpu.VMEM),
            scratch_shapes=[
                pltpu.VMEM((3 * ROWS, FEATS), BF16),
                pltpu.VMEM((RHS, 3 * ROWS), BF16),
                pltpu.VMEM((2 * ROWS, 128), BF16),
                pltpu.VMEM((3 * ROWS, 128), BF16),
                pltpu.VMEM((RHS, 2 * ROWS), F32),
                pltpu.VMEM((CHUNKS, RHS, STEP_C), F32),
                pltpu.VMEM((RHS, ROWS), F32),
                pltpu.VMEM((CHUNKS, RHS, STEP_C), F32),
                pltpu.VMEM((CHUNKS, RELAY_MAX, FEATS), BF16),
                pltpu.VMEM((STEP_R, STEP_C), BF16),
                pltpu.VMEM((STEP_R, STEP_C), BF16),
                dma((2,)), pltpu.SemaphoreType.REGULAR, dma((3,)), dma((3,)),
            ] + [dma((CHUNKS,))] * 10,
            compiler_params=pltpu.CompilerParams(
                collective_id=0, has_side_effects=True, vmem_limit_bytes=40 * 2**20),
        )(pltpu.with_memory_space_constraint(x_loc, pltpu.HBM), pltpu.with_memory_space_constraint(v_loc.T, pltpu.HBM), lengthscale, outscale)
        return y_t.T

    return jax.shard_map(local_fn, mesh=mesh, in_specs=(row_spec, row_spec, P(None), P(None)), out_specs=row_spec,
                         check_vma=False)
```

```python
import functools

import jax
import jax.numpy as jnp
from jax import lax
from jax.experimental import pallas as pl
from jax.experimental.pallas import tpu as pltpu
from jax.sharding import PartitionSpec as P

MESH = pl.DeviceIdType.MESH
F32 = jnp.float32
BF16 = jnp.bfloat16
LOG2E = 1.4426950408889634
ROWS, FEATS, RHS = 2048, 384, 32
STEP_R, STEP_C, SUB = 1024, 256, 256
CHUNKS = ROWS // STEP_C
DIRECT = (176,) * 8
RELAY_MAX = STEP_C - min(DIRECT)
OWN, SIB, FAR = 0, ROWS, 2 * ROWS
LENT = 2

PASS_OWN = (0,)
PASS_BOTH = ((1,), (2,), (3,))
PASS_FAR = ((4,), (5,), (6,), (7,), (), (), (), ())

NT = (((1,), (1,)), ((), ()))


def kernel(x_hbm, v_hbm, ell_ref, s_ref, out_ref,
           pts, vec, left, right, yloc, yfar, ysib, yret, relay, ka, kb,
           loc_sem, go_sem, sib_send, sib_recv, dir_send, dir_recv, dirv_send, dirv_recv,
           hop_send, hop_recv, fwd_send, fwd_recv, ret_send, ret_recv):
    t = lax.axis_index('tasks')
    g = lax.axis_index('group')
    core = lax.rem(g, 2)
    heavy = lax.div(g, 2) == t
    light = jnp.logical_not(heavy)
    g_sib = g + 1 - 2 * core
    g_far = lax.rem(g + 2, 4)
    t_other = 1 - t

    load_x = pltpu.make_async_copy(x_hbm, pts.at[pl.ds(OWN, ROWS)], loc_sem.at[0])
    load_v = pltpu.make_async_copy(v_hbm, vec.at[:, pl.ds(OWN, ROWS)], loc_sem.at[1])
    load_x.start()
    load_v.start()
    barrier = pltpu.get_barrier_semaphore()
    far_sib = lax.rem(g_sib + 2, 4)

    def greet(*devices):
        for dev in devices:
            pl.semaphore_signal(barrier, inc=1, device_id=dev, device_id_type=MESH)

    @pl.when(heavy)
    def _():
        greet((t, g_far), (t_other, g), (t, g_sib), (t_other, g_far))

    @pl.when(light)
    def _():
        greet((t, g_far), (t_other, g), (t, far_sib))

    def remote(src, dst, send, recv, dev):
        return pltpu.make_async_remote_copy(src_ref=src, dst_ref=dst, send_sem=send, recv_sem=recv,
                                            device_id=dev, device_id_type=MESH)

    def direct_x(k):
        lo, n = k * STEP_C, DIRECT[k]
        return remote(x_hbm.at[pl.ds(lo, n)], pts.at[pl.ds(FAR + lo, n)], dir_send.at[k], dir_recv.at[k], (t, g_far))

    def lent_x(k):
        at = pl.ds(k * STEP_C, STEP_C)
        return remote(x_hbm.at[at], pts.at[pl.ds(FAR + k * STEP_C, STEP_C)], dir_send.at[k], dir_recv.at[k], (t, g_far))

    def direct_v(k):
        lo = k * STEP_C
        return remote(v_hbm.at[:, pl.ds(lo, STEP_C)], vec.at[:, pl.ds(FAR + lo, STEP_C)],
                      dirv_send.at[k], dirv_recv.at[k], (t, g_far))

    def hop(k):
        lo, n = k * STEP_C + DIRECT[k], STEP_C - DIRECT[k]
        return remote(x_hbm.at[pl.ds(lo, n)], relay.at[k, pl.ds(0, n)], hop_send.at[k], hop_recv.at[k], (t_other, g))

    def forward(k):
        lo, n = k * STEP_C + DIRECT[k], STEP_C - DIRECT[k]
        return remote(relay.at[k, pl.ds(0, n)], pts.at[pl.ds(FAR + lo, n)], fwd_send.at[k], fwd_recv.at[k],
                      (t_other, g_far))

    def give_back(k):
        return remote(yfar.at[k], yret.at[k], ret_send.at[k], ret_recv.at[k], (t, g_far))

    sib_x = remote(x_hbm, pts.at[pl.ds(SIB, ROWS)], sib_send.at[0], sib_recv.at[0], (t, g_sib))
    sib_v = remote(v_hbm, vec.at[:, pl.ds(SIB, ROWS)], sib_send.at[1], sib_recv.at[1], (t, g_sib))
    sib_y = remote(yloc.at[:, pl.ds(SIB, ROWS)], ysib, sib_send.at[2], sib_recv.at[2], (t, g_sib))

    @pl.when(light)
    def _():
        pl.semaphore_wait(barrier, 2)
        for k in range(CHUNKS):
            direct_x(k).start()
            direct_v(k).start()
            hop(k).start()

    yloc[...] = jnp.zeros_like(yloc)
    yfar[...] = jnp.zeros_like(yfar)
    kb[...] = jnp.zeros_like(kb)
    ell = ell_ref[0]
    scale = s_ref[0]
    rate = -LOG2E / jnp.full((1, STEP_C), 2.0 * (ell * ell), F32)

    def split(n):
        high = n.astype(BF16).astype(F32)
        mid = (n - high).astype(BF16).astype(F32)
        return high, mid, (n - high) - mid

    def pick(index, parts):
        out = jnp.zeros_like(parts[0])
        for i, part in enumerate(parts):
            out = jnp.where(index == i, part, out)
        return out.astype(BF16)

    def norms(off, n, with_left):
        lane = lax.broadcasted_iota(jnp.int32, (128, 128), 1)
        one = jnp.ones((128, 128), F32)
        for lo in range(0, n, 128):
            rows = pl.ds(pl.multiple_of(off + lo, 128), 128)
            x = pts[rows, :].astype(F32)
            parts = split(jnp.broadcast_to(jnp.sum(x * x, axis=1, keepdims=True), (128, 128)))
            if with_left:
                left[rows, :] = pick(lane, (*parts, one, one, one))
            right[rows, :] = pick(lane, (one, one, one, *parts))

    def all_norms(off):
        def some(i, _):
            norms(off + i * 256, 256, True)
            return 0
        lax.fori_loop(0, ROWS // 256, some, 0)

    def apply_k(k_buf, q, row, col, both):
        blk = k_buf[pl.ds(q * SUB, SUB), :]
        at = pl.ds(pl.multiple_of(row + q * SUB, SUB), SUB)
        yloc[:, at] += lax.dot_general(vec[:, pl.ds(col, STEP_C)], blk, NT, preferred_element_type=F32)
        if both:
            return jnp.dot(vec[:, at], blk, preferred_element_type=F32)
        return None

    def add_cols(col, acc, chunk):
        if chunk is None:
            yloc[:, pl.ds(col, STEP_C)] += acc
        else:
            yfar[chunk] += acc

    def columns(col):
        at = pl.ds(col, STEP_C)
        return jnp.concatenate([pts[at, :] * BF16(-2.0), right[at, :]], axis=1)

    def step(slot, row, xr, prev_row, prev_col, both, prev_chunk):
        new, old = (ka, kb) if slot == 0 else (kb, ka)
        row, subs = row
        prev_row, prev_subs = prev_row
        acc = None
        for q in range(max(subs, prev_subs)):
            if q < subs:
                at = pl.ds(pl.multiple_of(row + q * SUB, SUB), SUB)
                xl = jnp.concatenate([pts[at, :], left[at, :]], axis=1)
                dist = jnp.maximum(lax.dot_general(xl, xr, NT, preferred_element_type=F32), 0.0)
                new[pl.ds(q * SUB, SUB), :] = (scale * jnp.exp2(dist * rate)).astype(BF16)
            if q < prev_subs:
                part = apply_k(old, q, prev_row, prev_col, both)
                if both:
                    acc = part if acc is None else acc + part
        if both:
            add_cols(prev_col, acc, prev_chunk)

    def drain(row, col, both, chunk):
        row, subs = row
        acc = None
        for q in range(subs):
            part = apply_k(kb, q, row, col, both)
            if both:
                acc = part if acc is None else acc + part
        if both:
            add_cols(col, acc, chunk)

    def tile_rows(x):
        return pl.multiple_of(x, STEP_C)

    load_x.wait()
    load_v.wait()
    all_norms(OWN)

    @pl.when(heavy)
    def _():
        pl.semaphore_wait(barrier, 5)
        pl.semaphore_signal(go_sem, inc=1, device_id=(t, g_far), device_id_type=MESH)
        for k in range(LENT):
            lent_x(k).start()
            direct_v(k).start()
        sib_x.start()
        sib_v.start()

    def diag_body(i, _):
        base = i * STEP_R
        before = jnp.maximum(i - 1, 0) * STEP_R
        for q in range(4):
            if q == 0:
                prev = ((tile_rows(before), 4), tile_rows(before + 3 * STEP_C))
            else:
                prev = ((tile_rows(base), 4), tile_rows(base + (q - 1) * STEP_C))
            step(q % 2, (tile_rows(base), 4), columns(tile_rows(base + q * STEP_C)), *prev, False, None)


        @pl.when(jnp.logical_and(light, i == 1))
        def _():
            pl.semaphore_wait(go_sem, 1)
            sib_x.start()
            sib_v.start()
        return 0

    lax.fori_loop(0, 2, diag_body, 0)
    drain((STEP_R, 4), STEP_R + 3 * STEP_C, False, None)
    kb[...] = jnp.zeros_like(kb)

    def pass_on(k):
        hop(k).wait_recv()
        forward(k).start()

    @pl.when(heavy)
    def _():
        for k in PASS_OWN:
            pass_on(k)

    sib_x.wait_recv()
    sib_v.wait_recv()
    all_norms(SIB)

    def both_place(i):
        row = jnp.where(i == 0, STEP_R, core * (SIB + STEP_R))
        col = jnp.where(i == 0, 0, jnp.where(core == 0, SIB, OWN) + (i - 1) * STEP_R)
        return row, col

    def both_body(i, _):
        @pl.when(heavy)
        def _():
            for at, some in enumerate(PASS_BOTH):
                @pl.when(i == at)
                def _():
                    for k in some:
                        pass_on(k)
        row, col = both_place(i)
        row0, col0 = both_place(jnp.maximum(i - 1, 0))
        for q in range(4):
            prev = ((tile_rows(row0), 4), tile_rows(col0 + 3 * STEP_C)) if q == 0 else (
                (tile_rows(row), 4), tile_rows(col + (q - 1) * STEP_C))
            step(q % 2, (tile_rows(row), 4), columns(tile_rows(col + q * STEP_C)), *prev, True, None)
        return 0

    lax.fori_loop(0, 3, both_body, 0)
    row_end, col_end = both_place(2)
    drain((tile_rows(row_end), 4), tile_rows(col_end + 3 * STEP_C), True, None)

    def far_pass(n, order, arrive):
        if n == 0:
            return
        kb[...] = jnp.zeros_like(kb)

        def far_body(k, _):
            for j in range(n):
                @pl.when(k == j)
                def _():
                    arrive(j)
            col = tile_rows(FAR + k * STEP_C)
            norms(col, STEP_C, False)
            xr = columns(col)
            before = jnp.maximum(k - 1, 0)
            for q in range(4):
                if q == 0:
                    step(0, order[0], xr, order[3], tile_rows(FAR + before * STEP_C), True, before)
                else:
                    step(q % 2, order[q], xr, order[q - 1], col, True, k)

            @pl.when(k > 0)
            def _():
                give_back(before).start()
            return 0

        lax.fori_loop(0, n, far_body, 0)
        drain(order[3], FAR + (n - 1) * STEP_C, True, n - 1)
        give_back(n - 1).start()

    def heavy_arrive(j):
        for k in PASS_FAR[j]:
            pass_on(k)
        direct_x(j).wait_recv()
        direct_v(j).wait_recv()
        forward(j).wait_recv()

    def light_arrive(j):
        lent_x(j).wait_recv()
        direct_v(j).wait_recv()

    def near_rows(first):
        subs = (ROWS - first) // SUB
        more = (subs + 1) // 2
        return [piece for base in (SIB, OWN)
                for piece in ((base + first, more), (base + first + more * SUB, subs - more))]

    @pl.when(heavy)
    def _():
        far_pass(CHUNKS, near_rows(LENT * STEP_C), heavy_arrive)

    @pl.when(light)
    def _():
        far_pass(LENT, near_rows(0), light_arrive)

    sib_y.start()
    sib_y.wait_recv()

    @pl.when(heavy)
    def _():
        for k in range(CHUNKS):
            at = pl.ds(k * STEP_C, STEP_C)
            total = yloc[:, at] + ysib[:, at]
            if k < LENT:
                give_back(k).wait_recv()
                total = total + yret[k]
            out_ref[:, at] = total
            forward(k).wait_send()
            give_back(k).wait_send()
        for k in range(LENT):
            lent_x(k).wait_send()
            direct_v(k).wait_send()

    @pl.when(light)
    def _():
        for k in range(CHUNKS):
            at = pl.ds(k * STEP_C, STEP_C)
            give_back(k).wait_recv()
            out_ref[:, at] = yloc[:, at] + ysib[:, at] + yret[k]
            direct_x(k).wait_send()
            direct_v(k).wait_send()
            hop(k).wait_send()
        for k in range(LENT):
            give_back(k).wait_send()

    sib_x.wait_send()
    sib_v.wait_send()
    sib_y.wait_send()


def solution(mesh):
    row_spec = P(('tasks', 'group'), None)
    dma = pltpu.SemaphoreType.DMA

    def local_fn(x_loc, v_loc, lengthscale, outscale):
        any_spec = pl.BlockSpec(memory_space=pl.ANY)
        smem = pl.BlockSpec(memory_space=pltpu.SMEM)
        y_t = pl.pallas_call(
            kernel,
            out_shape=jax.ShapeDtypeStruct((RHS, ROWS), F32),
            in_specs=[any_spec, any_spec, smem, smem],
            out_specs=pl.BlockSpec(memory_space=pltpu.VMEM),
            scratch_shapes=[
                pltpu.VMEM((3 * ROWS, FEATS), BF16),
                pltpu.VMEM((RHS, 3 * ROWS), BF16),
                pltpu.VMEM((2 * ROWS, 128), BF16),
                pltpu.VMEM((3 * ROWS, 128), BF16),
                pltpu.VMEM((RHS, 2 * ROWS), F32),
                pltpu.VMEM((CHUNKS, RHS, STEP_C), F32),
                pltpu.VMEM((RHS, ROWS), F32),
                pltpu.VMEM((CHUNKS, RHS, STEP_C), F32),
                pltpu.VMEM((CHUNKS, RELAY_MAX, FEATS), BF16),
                pltpu.VMEM((STEP_R, STEP_C), BF16),
                pltpu.VMEM((STEP_R, STEP_C), BF16),
                dma((2,)), pltpu.SemaphoreType.REGULAR, dma((3,)), dma((3,)),
            ] + [dma((CHUNKS,))] * 10,
            compiler_params=pltpu.CompilerParams(
                collective_id=0, has_side_effects=True, vmem_limit_bytes=40 * 2**20),
        )(pltpu.with_memory_space_constraint(x_loc, pltpu.HBM), pltpu.with_memory_space_constraint(v_loc.T, pltpu.HBM), lengthscale, outscale)
        return y_t.T

    return jax.shard_map(local_fn, mesh=mesh, in_specs=(row_spec, row_spec, P(None), P(None)), out_specs=row_spec,
                         check_vma=False)
```

```python
import functools

import jax
import jax.numpy as jnp
from jax import lax
from jax.experimental import pallas as pl
from jax.experimental.pallas import tpu as pltpu
from jax.sharding import PartitionSpec as P

MESH = pl.DeviceIdType.MESH
F32 = jnp.float32
BF16 = jnp.bfloat16
LOG2E = 1.4426950408889634
ROWS, FEATS, RHS = 2048, 384, 32
STEP_R, STEP_C, SUB = 1024, 256, 256
CHUNKS = ROWS // STEP_C
DIRECT = (160, 176) * 4
RELAY_MAX = STEP_C - min(DIRECT)
OWN, SIB, FAR = 0, ROWS, 2 * ROWS
LENT = 2

PASS_OWN = (0,)
PASS_BOTH = ((1,), (2,), ())
PASS_FAR = ((3,), (4,), (5,), (6,), (7,), (), (), ())

NT = (((1,), (1,)), ((), ()))


def kernel(x_hbm, v_hbm, ell_ref, s_ref, out_ref,
           pts, vec, left, right, yloc, yfar, ysib, yret, relay, ka, kb,
           loc_sem, go_sem, sib_send, sib_recv, dir_send, dir_recv, dirv_send, dirv_recv,
           hop_send, hop_recv, fwd_send, fwd_recv, ret_send, ret_recv):
    t = lax.axis_index('tasks')
    g = lax.axis_index('group')
    core = lax.rem(g, 2)
    heavy = lax.div(g, 2) == t
    light = jnp.logical_not(heavy)
    g_sib = g + 1 - 2 * core
    g_far = lax.rem(g + 2, 4)
    t_other = 1 - t

    load_x = pltpu.make_async_copy(x_hbm, pts.at[pl.ds(OWN, ROWS)], loc_sem.at[0])
    load_v = pltpu.make_async_copy(v_hbm, vec.at[:, pl.ds(OWN, ROWS)], loc_sem.at[1])
    load_x.start()
    load_v.start()
    barrier = pltpu.get_barrier_semaphore()
    far_sib = lax.rem(g_sib + 2, 4)

    def greet(*devices):
        for dev in devices:
            pl.semaphore_signal(barrier, inc=1, device_id=dev, device_id_type=MESH)

    @pl.when(heavy)
    def _():
        greet((t, g_far), (t_other, g), (t, g_sib), (t_other, g_far))

    @pl.when(light)
    def _():
        greet((t, g_far), (t_other, g), (t, far_sib))

    def remote(src, dst, send, recv, dev):
        return pltpu.make_async_remote_copy(src_ref=src, dst_ref=dst, send_sem=send, recv_sem=recv,
                                            device_id=dev, device_id_type=MESH)

    def direct_x(k):
        lo, n = k * STEP_C, DIRECT[k]
        return remote(x_hbm.at[pl.ds(lo, n)], pts.at[pl.ds(FAR + lo, n)], dir_send.at[k], dir_recv.at[k], (t, g_far))

    def lent_x(k):
        at = pl.ds(k * STEP_C, STEP_C)
        return remote(x_hbm.at[at], pts.at[pl.ds(FAR + k * STEP_C, STEP_C)], dir_send.at[k], dir_recv.at[k], (t, g_far))

    def direct_v(k):
        lo = k * STEP_C
        return remote(v_hbm.at[:, pl.ds(lo, STEP_C)], vec.at[:, pl.ds(FAR + lo, STEP_C)],
                      dirv_send.at[k], dirv_recv.at[k], (t, g_far))

    def hop(k):
        lo, n = k * STEP_C + DIRECT[k], STEP_C - DIRECT[k]
        return remote(x_hbm.at[pl.ds(lo, n)], relay.at[k, pl.ds(0, n)], hop_send.at[k], hop_recv.at[k], (t_other, g))

    def forward(k):
        lo, n = k * STEP_C + DIRECT[k], STEP_C - DIRECT[k]
        return remote(relay.at[k, pl.ds(0, n)], pts.at[pl.ds(FAR + lo, n)], fwd_send.at[k], fwd_recv.at[k],
                      (t_other, g_far))

    def give_back(k):
        return remote(yfar.at[k], yret.at[k], ret_send.at[k], ret_recv.at[k], (t, g_far))

    sib_x = remote(x_hbm, pts.at[pl.ds(SIB, ROWS)], sib_send.at[0], sib_recv.at[0], (t, g_sib))
    sib_v = remote(v_hbm, vec.at[:, pl.ds(SIB, ROWS)], sib_send.at[1], sib_recv.at[1], (t, g_sib))
    sib_y = remote(yloc.at[:, pl.ds(SIB, ROWS)], ysib, sib_send.at[2], sib_recv.at[2], (t, g_sib))

    @pl.when(light)
    def _():
        pl.semaphore_wait(barrier, 2)
        for k in range(CHUNKS):
            direct_x(k).start()
            direct_v(k).start()
            hop(k).start()

    yloc[...] = jnp.zeros_like(yloc)
    yfar[...] = jnp.zeros_like(yfar)
    kb[...] = jnp.zeros_like(kb)
    ell = ell_ref[0]
    scale = s_ref[0]
    rate = -LOG2E / jnp.full((1, STEP_C), 2.0 * (ell * ell), F32)

    def split(n):
        high = n.astype(BF16).astype(F32)
        mid = (n - high).astype(BF16).astype(F32)
        return high, mid, (n - high) - mid

    def pick(index, parts):
        out = jnp.zeros_like(parts[0])
        for i, part in enumerate(parts):
            out = jnp.where(index == i, part, out)
        return out.astype(BF16)

    def norms(off, n, with_left):
        lane = lax.broadcasted_iota(jnp.int32, (128, 128), 1)
        one = jnp.ones((128, 128), F32)
        for lo in range(0, n, 128):
            rows = pl.ds(pl.multiple_of(off + lo, 128), 128)
            x = pts[rows, :].astype(F32)
            parts = split(jnp.broadcast_to(jnp.sum(x * x, axis=1, keepdims=True), (128, 128)))
            if with_left:
                left[rows, :] = pick(lane, (*parts, one, one, one))
            right[rows, :] = pick(lane, (one, one, one, *parts))

    def all_norms(off):
        def some(i, _):
            norms(off + i * 256, 256, True)
            return 0
        lax.fori_loop(0, ROWS // 256, some, 0)

    def apply_k(k_buf, q, row, col, both):
        blk = k_buf[pl.ds(q * SUB, SUB), :]
        at = pl.ds(pl.multiple_of(row + q * SUB, SUB), SUB)
        yloc[:, at] += lax.dot_general(vec[:, pl.ds(col, STEP_C)], blk, NT, preferred_element_type=F32)
        if both:
            return jnp.dot(vec[:, at], blk, preferred_element_type=F32)
        return None

    def add_cols(col, acc, chunk):
        if chunk is None:
            yloc[:, pl.ds(col, STEP_C)] += acc
        else:
            yfar[chunk] += acc

    def columns(col):
        at = pl.ds(col, STEP_C)
        return jnp.concatenate([pts[at, :] * BF16(-2.0), right[at, :]], axis=1)

    def step(slot, row, xr, prev_row, prev_col, both, prev_chunk):
        new, old = (ka, kb) if slot == 0 else (kb, ka)
        row, subs = row
        prev_row, prev_subs = prev_row
        acc = None
        for q in range(max(subs, prev_subs)):
            if q < subs:
                at = pl.ds(pl.multiple_of(row + q * SUB, SUB), SUB)
                xl = jnp.concatenate([pts[at, :], left[at, :]], axis=1)
                dist = jnp.maximum(lax.dot_general(xl, xr, NT, preferred_element_type=F32), 0.0)
                new[pl.ds(q * SUB, SUB), :] = (scale * jnp.exp2(dist * rate)).astype(BF16)
            if q < prev_subs:
                part = apply_k(old, q, prev_row, prev_col, both)
                if both:
                    acc = part if acc is None else acc + part
        if both:
            add_cols(prev_col, acc, prev_chunk)

    def drain(row, col, both, chunk):
        row, subs = row
        acc = None
        for q in range(subs):
            part = apply_k(kb, q, row, col, both)
            if both:
                acc = part if acc is None else acc + part
        if both:
            add_cols(col, acc, chunk)

    def tile_rows(x):
        return pl.multiple_of(x, STEP_C)

    load_x.wait()
    load_v.wait()
    all_norms(OWN)

    @pl.when(heavy)
    def _():
        pl.semaphore_wait(barrier, 5)
        pl.semaphore_signal(go_sem, inc=1, device_id=(t, g_far), device_id_type=MESH)
        for k in range(LENT):
            lent_x(k).start()
            direct_v(k).start()
        sib_x.start()
        sib_v.start()

    def diag_body(i, _):
        base = i * STEP_R
        before = jnp.maximum(i - 1, 0) * STEP_R
        for q in range(4):
            if q == 0:
                prev = ((tile_rows(before), 4), tile_rows(before + 3 * STEP_C))
            else:
                prev = ((tile_rows(base), 4), tile_rows(base + (q - 1) * STEP_C))
            step(q % 2, (tile_rows(base), 4), columns(tile_rows(base + q * STEP_C)), *prev, False, None)


        @pl.when(jnp.logical_and(light, i == 1))
        def _():
            pl.semaphore_wait(go_sem, 1)
            sib_x.start()
            sib_v.start()
        return 0

    lax.fori_loop(0, 2, diag_body, 0)
    drain((STEP_R, 4), STEP_R + 3 * STEP_C, False, None)
    kb[...] = jnp.zeros_like(kb)

    def pass_on(k):
        hop(k).wait_recv()
        forward(k).start()

    @pl.when(heavy)
    def _():
        for k in PASS_OWN:
            pass_on(k)

    sib_x.wait_recv()
    sib_v.wait_recv()
    all_norms(SIB)

    def both_place(i):
        row = jnp.where(i == 0, STEP_R, core * (SIB + STEP_R))
        col = jnp.where(i == 0, 0, jnp.where(core == 0, SIB, OWN) + (i - 1) * STEP_R)
        return row, col

    def both_body(i, _):
        @pl.when(heavy)
        def _():
            for at, some in enumerate(PASS_BOTH):
                @pl.when(i == at)
                def _():
                    for k in some:
                        pass_on(k)
        row, col = both_place(i)
        row0, col0 = both_place(jnp.maximum(i - 1, 0))
        for q in range(4):
            prev = ((tile_rows(row0), 4), tile_rows(col0 + 3 * STEP_C)) if q == 0 else (
                (tile_rows(row), 4), tile_rows(col + (q - 1) * STEP_C))
            step(q % 2, (tile_rows(row), 4), columns(tile_rows(col + q * STEP_C)), *prev, True, None)
        return 0

    lax.fori_loop(0, 3, both_body, 0)
    row_end, col_end = both_place(2)
    drain((tile_rows(row_end), 4), tile_rows(col_end + 3 * STEP_C), True, None)

    def far_pass(n, order, arrive):
        if n == 0:
            return
        kb[...] = jnp.zeros_like(kb)

        def far_body(k, _):
            for j in range(n):
                @pl.when(k == j)
                def _():
                    arrive(j)
            col = tile_rows(FAR + k * STEP_C)
            norms(col, STEP_C, False)
            xr = columns(col)
            before = jnp.maximum(k - 1, 0)
            for q in range(4):
                if q == 0:
                    step(0, order[0], xr, order[3], tile_rows(FAR + before * STEP_C), True, before)
                else:
                    step(q % 2, order[q], xr, order[q - 1], col, True, k)

            @pl.when(k > 0)
            def _():
                give_back(before).start()
            return 0

        lax.fori_loop(0, n, far_body, 0)
        drain(order[3], FAR + (n - 1) * STEP_C, True, n - 1)
        give_back(n - 1).start()

    def heavy_arrive(j):
        for k in PASS_FAR[j]:
            pass_on(k)
        direct_x(j).wait_recv()
        direct_v(j).wait_recv()
        forward(j).wait_recv()

    def light_arrive(j):
        lent_x(j).wait_recv()
        direct_v(j).wait_recv()

    def near_rows(first):
        subs = (ROWS - first) // SUB
        more = (subs + 1) // 2
        return [piece for base in (SIB, OWN)
                for piece in ((base + first, more), (base + first + more * SUB, subs - more))]

    @pl.when(heavy)
    def _():
        far_pass(CHUNKS, near_rows(LENT * STEP_C), heavy_arrive)

    @pl.when(light)
    def _():
        far_pass(LENT, near_rows(0), light_arrive)

    sib_y.start()
    sib_y.wait_recv()

    @pl.when(heavy)
    def _():
        for k in range(CHUNKS):
            at = pl.ds(k * STEP_C, STEP_C)
            total = yloc[:, at] + ysib[:, at]
            if k < LENT:
                give_back(k).wait_recv()
                total = total + yret[k]
            out_ref[:, at] = total
            forward(k).wait_send()
            give_back(k).wait_send()
        for k in range(LENT):
            lent_x(k).wait_send()
            direct_v(k).wait_send()

    @pl.when(light)
    def _():
        for k in range(CHUNKS):
            at = pl.ds(k * STEP_C, STEP_C)
            give_back(k).wait_recv()
            out_ref[:, at] = yloc[:, at] + ysib[:, at] + yret[k]
            direct_x(k).wait_send()
            direct_v(k).wait_send()
            hop(k).wait_send()
        for k in range(LENT):
            give_back(k).wait_send()

    sib_x.wait_send()
    sib_v.wait_send()
    sib_y.wait_send()


def solution(mesh):
    row_spec = P(('tasks', 'group'), None)
    dma = pltpu.SemaphoreType.DMA

    def local_fn(x_loc, v_loc, lengthscale, outscale):
        any_spec = pl.BlockSpec(memory_space=pl.ANY)
        smem = pl.BlockSpec(memory_space=pltpu.SMEM)
        y_t = pl.pallas_call(
            kernel,
            out_shape=jax.ShapeDtypeStruct((RHS, ROWS), F32),
            in_specs=[any_spec, any_spec, smem, smem],
            out_specs=pl.BlockSpec(memory_space=pltpu.VMEM),
            scratch_shapes=[
                pltpu.VMEM((3 * ROWS, FEATS), BF16),
                pltpu.VMEM((RHS, 3 * ROWS), BF16),
                pltpu.VMEM((2 * ROWS, 128), BF16),
                pltpu.VMEM((3 * ROWS, 128), BF16),
                pltpu.VMEM((RHS, 2 * ROWS), F32),
                pltpu.VMEM((CHUNKS, RHS, STEP_C), F32),
                pltpu.VMEM((RHS, ROWS), F32),
                pltpu.VMEM((CHUNKS, RHS, STEP_C), F32),
                pltpu.VMEM((CHUNKS, RELAY_MAX, FEATS), BF16),
                pltpu.VMEM((STEP_R, STEP_C), BF16),
                pltpu.VMEM((STEP_R, STEP_C), BF16),
                dma((2,)), pltpu.SemaphoreType.REGULAR, dma((3,)), dma((3,)),
            ] + [dma((CHUNKS,))] * 10,
            compiler_params=pltpu.CompilerParams(
                collective_id=0, has_side_effects=True, vmem_limit_bytes=40 * 2**20),
        )(pltpu.with_memory_space_constraint(x_loc, pltpu.HBM), pltpu.with_memory_space_constraint(v_loc.T, pltpu.HBM), lengthscale, outscale)
        return y_t.T

    return jax.shard_map(local_fn, mesh=mesh, in_specs=(row_spec, row_spec, P(None), P(None)), out_specs=row_spec,
                         check_vma=False)
```

```python
import functools

import jax
import jax.numpy as jnp
from jax import lax
from jax.experimental import pallas as pl
from jax.experimental.pallas import tpu as pltpu
from jax.sharding import PartitionSpec as P

MESH = pl.DeviceIdType.MESH
F32 = jnp.float32
BF16 = jnp.bfloat16
LOG2E = 1.4426950408889634
ROWS, FEATS, RHS = 2048, 384, 32
STEP_R, STEP_C, SUB = 1024, 256, 256
CHUNKS = ROWS // STEP_C
DIRECT = (160, 176) * 4
RELAY_MAX = STEP_C - min(DIRECT)
OWN, SIB, FAR = 0, ROWS, 2 * ROWS
LENT = 2

PASS_OWN = (0,)
PASS_BOTH = ((1,), (2,), ())
PASS_FAR = ((3,), (4,), (5,), (6,), (7,), (), (), ())

NT = (((1,), (1,)), ((), ()))


def kernel(x_hbm, v_hbm, ell_ref, s_ref, out_ref,
           pts, vec, left, right, yloc, yfar, ysib, yret, relay, ka, kb,
           loc_sem, go_sem, sib_send, sib_recv, dir_send, dir_recv, dirv_send, dirv_recv,
           hop_send, hop_recv, fwd_send, fwd_recv, ret_send, ret_recv):
    t = lax.axis_index('tasks')
    g = lax.axis_index('group')
    core = lax.rem(g, 2)
    heavy = lax.div(g, 2) == t
    light = jnp.logical_not(heavy)
    g_sib = g + 1 - 2 * core
    g_far = lax.rem(g + 2, 4)
    t_other = 1 - t

    load_x = pltpu.make_async_copy(x_hbm, pts.at[pl.ds(OWN, ROWS)], loc_sem.at[0])
    load_v = pltpu.make_async_copy(v_hbm, vec.at[:, pl.ds(OWN, ROWS)], loc_sem.at[1])
    load_x.start()
    load_v.start()
    barrier = pltpu.get_barrier_semaphore()
    far_sib = lax.rem(g_sib + 2, 4)

    def greet(*devices):
        for dev in devices:
            pl.semaphore_signal(barrier, inc=1, device_id=dev, device_id_type=MESH)

    @pl.when(heavy)
    def _():
        greet((t, g_far), (t_other, g), (t, g_sib), (t_other, g_far))

    @pl.when(light)
    def _():
        greet((t, g_far), (t_other, g), (t, far_sib))

    def remote(src, dst, send, recv, dev):
        return pltpu.make_async_remote_copy(src_ref=src, dst_ref=dst, send_sem=send, recv_sem=recv,
                                            device_id=dev, device_id_type=MESH)

    def direct_x(k):
        lo, n = k * STEP_C, DIRECT[k]
        return remote(x_hbm.at[pl.ds(lo, n)], pts.at[pl.ds(FAR + lo, n)], dir_send.at[k], dir_recv.at[k], (t, g_far))

    def lent_x(k):
        at = pl.ds(k * STEP_C, STEP_C)
        return remote(x_hbm.at[at], pts.at[pl.ds(FAR + k * STEP_C, STEP_C)], dir_send.at[k], dir_recv.at[k], (t, g_far))

    def direct_v(k):
        lo = k * STEP_C
        return remote(v_hbm.at[:, pl.ds(lo, STEP_C)], vec.at[:, pl.ds(FAR + lo, STEP_C)],
                      dirv_send.at[k], dirv_recv.at[k], (t, g_far))

    def hop(k):
        lo, n = k * STEP_C + DIRECT[k], STEP_C - DIRECT[k]
        return remote(x_hbm.at[pl.ds(lo, n)], relay.at[k, pl.ds(0, n)], hop_send.at[k], hop_recv.at[k], (t_other, g))

    def forward(k):
        lo, n = k * STEP_C + DIRECT[k], STEP_C - DIRECT[k]
        return remote(relay.at[k, pl.ds(0, n)], pts.at[pl.ds(FAR + lo, n)], fwd_send.at[k], fwd_recv.at[k],
                      (t_other, g_far))

    def give_back(k):
        return remote(yfar.at[k], yret.at[k], ret_send.at[k], ret_recv.at[k], (t, g_far))

    sib_x = remote(x_hbm, pts.at[pl.ds(SIB, ROWS)], sib_send.at[0], sib_recv.at[0], (t, g_sib))
    sib_v = remote(v_hbm, vec.at[:, pl.ds(SIB, ROWS)], sib_send.at[1], sib_recv.at[1], (t, g_sib))
    sib_y = remote(yloc.at[:, pl.ds(SIB, ROWS)], ysib, sib_send.at[2], sib_recv.at[2], (t, g_sib))

    @pl.when(light)
    def _():
        pl.semaphore_wait(barrier, 2)
        for k in range(CHUNKS):
            direct_x(k).start()
            direct_v(k).start()
            hop(k).start()

    yloc[...] = jnp.zeros_like(yloc)
    yfar[...] = jnp.zeros_like(yfar)
    kb[...] = jnp.zeros_like(kb)
    ell = ell_ref[0]
    scale = s_ref[0]
    rate = -LOG2E / jnp.full((1, STEP_C), 2.0 * (ell * ell), F32)

    def split(n):
        high = n.astype(BF16).astype(F32)
        mid = (n - high).astype(BF16).astype(F32)
        return high, mid, (n - high) - mid

    def pick(index, parts):
        out = jnp.zeros_like(parts[0])
        for i, part in enumerate(parts):
            out = jnp.where(index == i, part, out)
        return out.astype(BF16)

    def norms(off, n, with_left):
        lane = lax.broadcasted_iota(jnp.int32, (128, 128), 1)
        one = jnp.ones((128, 128), F32)
        for lo in range(0, n, 128):
            rows = pl.ds(pl.multiple_of(off + lo, 128), 128)
            x = pts[rows, :].astype(F32)
            parts = split(jnp.broadcast_to(jnp.sum(x * x, axis=1, keepdims=True), (128, 128)))
            if with_left:
                left[rows, :] = pick(lane, (*parts, one, one, one))
            right[rows, :] = pick(lane, (one, one, one, *parts))

    def all_norms(off):
        def some(i, _):
            norms(off + i * 256, 256, True)
            return 0
        lax.fori_loop(0, ROWS // 256, some, 0)

    def apply_k(k_buf, q, row, col, both):
        blk = k_buf[pl.ds(q * SUB, SUB), :]
        at = pl.ds(pl.multiple_of(row + q * SUB, SUB), SUB)
        yloc[:, at] += lax.dot_general(vec[:, pl.ds(col, STEP_C)], blk, NT, preferred_element_type=F32)
        if both:
            return jnp.dot(vec[:, at], blk, preferred_element_type=F32)
        return None

    def add_cols(col, acc, chunk):
        if chunk is None:
            yloc[:, pl.ds(col, STEP_C)] += acc
        else:
            yfar[chunk] += acc

    def columns(col):
        at = pl.ds(col, STEP_C)
        return jnp.concatenate([pts[at, :] * BF16(-2.0), right[at, :]], axis=1)

    def step(slot, row, xr, prev_row, prev_col, both, prev_chunk):
        new, old = (ka, kb) if slot == 0 else (kb, ka)
        row, subs = row
        prev_row, prev_subs = prev_row
        acc = None
        for q in range(max(subs, prev_subs)):
            if q < subs:
                at = pl.ds(pl.multiple_of(row + q * SUB, SUB), SUB)
                xl = jnp.concatenate([pts[at, :], left[at, :]], axis=1)
                dist = jnp.maximum(lax.dot_general(xl, xr, NT, preferred_element_type=F32), 0.0)
                new[pl.ds(q * SUB, SUB), :] = (scale * jnp.exp2(dist * rate)).astype(BF16)
            if q < prev_subs:
                part = apply_k(old, q, prev_row, prev_col, both)
                if both:
                    acc = part if acc is None else acc + part
        if both:
            add_cols(prev_col, acc, prev_chunk)

    def drain(row, col, both, chunk):
        row, subs = row
        acc = None
        for q in range(subs):
            part = apply_k(kb, q, row, col, both)
            if both:
                acc = part if acc is None else acc + part
        if both:
            add_cols(col, acc, chunk)

    def tile_rows(x):
        return pl.multiple_of(x, STEP_C)

    load_x.wait()
    load_v.wait()
    all_norms(OWN)

    @pl.when(heavy)
    def _():
        pl.semaphore_wait(barrier, 5)
        pl.semaphore_signal(go_sem, inc=1, device_id=(t, g_far), device_id_type=MESH)
        for k in range(LENT):
            lent_x(k).start()
            direct_v(k).start()
        sib_x.start()
        sib_v.start()

    def diag_body(i, _):
        base = i * STEP_R
        before = jnp.maximum(i - 1, 0) * STEP_R
        for q in range(4):
            if q == 0:
                prev = ((tile_rows(before), 4), tile_rows(before + 3 * STEP_C))
            else:
                prev = ((tile_rows(base), 4), tile_rows(base + (q - 1) * STEP_C))
            step(q % 2, (tile_rows(base), 4), columns(tile_rows(base + q * STEP_C)), *prev, False, None)


        @pl.when(jnp.logical_and(light, i == 1))
        def _():
            pl.semaphore_wait(go_sem, 1)
            sib_x.start()
            sib_v.start()
        return 0

    lax.fori_loop(0, 2, diag_body, 0)
    drain((STEP_R, 4), STEP_R + 3 * STEP_C, False, None)
    kb[...] = jnp.zeros_like(kb)

    def pass_on(k):
        hop(k).wait_recv()
        forward(k).start()

    @pl.when(heavy)
    def _():
        for k in PASS_OWN:
            pass_on(k)

    sib_x.wait_recv()
    sib_v.wait_recv()
    all_norms(SIB)

    def both_place(i):
        row = jnp.where(i == 0, STEP_R, core * (SIB + STEP_R))
        col = jnp.where(i == 0, 0, jnp.where(core == 0, SIB, OWN) + (i - 1) * STEP_R)
        return row, col

    def both_body(i, _):
        @pl.when(heavy)
        def _():
            for at, some in enumerate(PASS_BOTH):
                @pl.when(i == at)
                def _():
                    for k in some:
                        pass_on(k)
        row, col = both_place(i)
        row0, col0 = both_place(jnp.maximum(i - 1, 0))
        for q in range(4):
            prev = ((tile_rows(row0), 4), tile_rows(col0 + 3 * STEP_C)) if q == 0 else (
                (tile_rows(row), 4), tile_rows(col + (q - 1) * STEP_C))
            step(q % 2, (tile_rows(row), 4), columns(tile_rows(col + q * STEP_C)), *prev, True, None)
        return 0

    lax.fori_loop(0, 3, both_body, 0)
    row_end, col_end = both_place(2)
    drain((tile_rows(row_end), 4), tile_rows(col_end + 3 * STEP_C), True, None)

    def far_pass(n, order, arrive):
        if n == 0:
            return
        kb[...] = jnp.zeros_like(kb)

        def far_body(k, _):
            for j in range(n):
                @pl.when(k == j)
                def _():
                    arrive(j)
            col = tile_rows(FAR + k * STEP_C)
            norms(col, STEP_C, False)
            xr = columns(col)
            before = jnp.maximum(k - 1, 0)
            for q in range(4):
                if q == 0:
                    step(0, order[0], xr, order[3], tile_rows(FAR + before * STEP_C), True, before)
                else:
                    step(q % 2, order[q], xr, order[q - 1], col, True, k)

            @pl.when(k > 0)
            def _():
                give_back(before).start()
            return 0

        lax.fori_loop(0, n, far_body, 0)
        sib_y.start()
        drain(order[3], FAR + (n - 1) * STEP_C, True, n - 1)
        give_back(n - 1).start()

    def heavy_arrive(j):
        for k in PASS_FAR[j]:
            pass_on(k)
        direct_x(j).wait_recv()
        direct_v(j).wait_recv()
        forward(j).wait_recv()

    def light_arrive(j):
        lent_x(j).wait_recv()
        direct_v(j).wait_recv()

    def near_rows(first):
        subs = (ROWS - first) // SUB
        return [piece for base, more in ((SIB, (subs + 1) // 2), (OWN, 4))
                for piece in ((base + first, more), (base + first + more * SUB, subs - more))]

    @pl.when(heavy)
    def _():
        far_pass(CHUNKS, near_rows(LENT * STEP_C), heavy_arrive)

    @pl.when(light)
    def _():
        far_pass(LENT, near_rows(0), light_arrive)

    sib_y.wait_recv()

    @pl.when(heavy)
    def _():
        for k in range(CHUNKS):
            at = pl.ds(k * STEP_C, STEP_C)
            total = yloc[:, at] + ysib[:, at]
            if k < LENT:
                give_back(k).wait_recv()
                total = total + yret[k]
            out_ref[:, at] = total
            forward(k).wait_send()
            give_back(k).wait_send()
        for k in range(LENT):
            lent_x(k).wait_send()
            direct_v(k).wait_send()

    @pl.when(light)
    def _():
        for k in range(CHUNKS):
            at = pl.ds(k * STEP_C, STEP_C)
            give_back(k).wait_recv()
            out_ref[:, at] = yloc[:, at] + ysib[:, at] + yret[k]
            direct_x(k).wait_send()
            direct_v(k).wait_send()
            hop(k).wait_send()
        for k in range(LENT):
            give_back(k).wait_send()

    sib_x.wait_send()
    sib_v.wait_send()
    sib_y.wait_send()


def solution(mesh):
    row_spec = P(('tasks', 'group'), None)
    dma = pltpu.SemaphoreType.DMA

    def local_fn(x_loc, v_loc, lengthscale, outscale):
        any_spec = pl.BlockSpec(memory_space=pl.ANY)
        smem = pl.BlockSpec(memory_space=pltpu.SMEM)
        y_t = pl.pallas_call(
            kernel,
            out_shape=jax.ShapeDtypeStruct((RHS, ROWS), F32),
            in_specs=[any_spec, any_spec, smem, smem],
            out_specs=pl.BlockSpec(memory_space=pltpu.VMEM),
            scratch_shapes=[
                pltpu.VMEM((3 * ROWS, FEATS), BF16),
                pltpu.VMEM((RHS, 3 * ROWS), BF16),
                pltpu.VMEM((2 * ROWS, 128), BF16),
                pltpu.VMEM((3 * ROWS, 128), BF16),
                pltpu.VMEM((RHS, 2 * ROWS), F32),
                pltpu.VMEM((CHUNKS, RHS, STEP_C), F32),
                pltpu.VMEM((RHS, ROWS), F32),
                pltpu.VMEM((CHUNKS, RHS, STEP_C), F32),
                pltpu.VMEM((CHUNKS, RELAY_MAX, FEATS), BF16),
                pltpu.VMEM((STEP_R, STEP_C), BF16),
                pltpu.VMEM((STEP_R, STEP_C), BF16),
                dma((2,)), pltpu.SemaphoreType.REGULAR, dma((3,)), dma((3,)),
            ] + [dma((CHUNKS,))] * 10,
            compiler_params=pltpu.CompilerParams(
                collective_id=0, has_side_effects=True, vmem_limit_bytes=40 * 2**20),
        )(pltpu.with_memory_space_constraint(x_loc, pltpu.HBM), pltpu.with_memory_space_constraint(v_loc.T, pltpu.HBM), lengthscale, outscale)
        return y_t.T

    return jax.shard_map(local_fn, mesh=mesh, in_specs=(row_spec, row_spec, P(None), P(None)), out_specs=row_spec,
                         check_vma=False)
```

```python
import functools

import jax
import jax.numpy as jnp
from jax import lax
from jax.experimental import pallas as pl
from jax.experimental.pallas import tpu as pltpu
from jax.sharding import PartitionSpec as P

MESH = pl.DeviceIdType.MESH
F32 = jnp.float32
BF16 = jnp.bfloat16
LOG2E = 1.4426950408889634
ROWS, FEATS, RHS = 2048, 384, 32
STEP_R, STEP_C, SUB = 1024, 256, 256
CHUNKS = ROWS // STEP_C
DIRECT = (160, 176) * 4
RELAY_MAX = STEP_C - min(DIRECT)
OWN, SIB, FAR = 0, ROWS, 2 * ROWS
LENT = 2

PASS_OWN = (0,)
PASS_BOTH = ((1,), (2,), ())
PASS_FAR = ((3,), (4,), (5,), (6,), (7,), (), (), ())

NT = (((1,), (1,)), ((), ()))


def kernel(x_hbm, v_hbm, ell_ref, s_ref, out_ref,
           pts, vec, left, right, yloc, yfar, ysib, yret, relay, ka, kb,
           loc_sem, go_sem, sib_send, sib_recv, dir_send, dir_recv, dirv_send, dirv_recv,
           hop_send, hop_recv, fwd_send, fwd_recv, ret_send, ret_recv):
    t = lax.axis_index('tasks')
    g = lax.axis_index('group')
    core = lax.rem(g, 2)
    heavy = lax.div(g, 2) == t
    light = jnp.logical_not(heavy)
    g_sib = g + 1 - 2 * core
    g_far = lax.rem(g + 2, 4)
    t_other = 1 - t

    load_x = pltpu.make_async_copy(x_hbm, pts.at[pl.ds(OWN, ROWS)], loc_sem.at[0])
    load_v = pltpu.make_async_copy(v_hbm, vec.at[:, pl.ds(OWN, ROWS)], loc_sem.at[1])
    load_x.start()
    load_v.start()
    barrier = pltpu.get_barrier_semaphore()
    far_sib = lax.rem(g_sib + 2, 4)

    def greet(*devices):
        for dev in devices:
            pl.semaphore_signal(barrier, inc=1, device_id=dev, device_id_type=MESH)

    @pl.when(heavy)
    def _():
        greet((t, g_far), (t_other, g), (t, g_sib), (t_other, g_far))

    @pl.when(light)
    def _():
        greet((t, g_far), (t_other, g), (t, far_sib))

    def remote(src, dst, send, recv, dev):
        return pltpu.make_async_remote_copy(src_ref=src, dst_ref=dst, send_sem=send, recv_sem=recv,
                                            device_id=dev, device_id_type=MESH)

    def direct_x(k):
        lo, n = k * STEP_C, DIRECT[k]
        return remote(x_hbm.at[pl.ds(lo, n)], pts.at[pl.ds(FAR + lo, n)], dir_send.at[k], dir_recv.at[k], (t, g_far))

    def lent_x(k):
        at = pl.ds(k * STEP_C, STEP_C)
        return remote(x_hbm.at[at], pts.at[pl.ds(FAR + k * STEP_C, STEP_C)], dir_send.at[k], dir_recv.at[k], (t, g_far))

    def direct_v(k):
        lo = k * STEP_C
        return remote(v_hbm.at[:, pl.ds(lo, STEP_C)], vec.at[:, pl.ds(FAR + lo, STEP_C)],
                      dirv_send.at[k], dirv_recv.at[k], (t, g_far))

    def hop(k):
        lo, n = k * STEP_C + DIRECT[k], STEP_C - DIRECT[k]
        return remote(x_hbm.at[pl.ds(lo, n)], relay.at[k, pl.ds(0, n)], hop_send.at[k], hop_recv.at[k], (t_other, g))

    def forward(k):
        lo, n = k * STEP_C + DIRECT[k], STEP_C - DIRECT[k]
        return remote(relay.at[k, pl.ds(0, n)], pts.at[pl.ds(FAR + lo, n)], fwd_send.at[k], fwd_recv.at[k],
                      (t_other, g_far))

    def give_back(k):
        return remote(yfar.at[k], yret.at[k], ret_send.at[k], ret_recv.at[k], (t, g_far))

    sib_x = remote(x_hbm, pts.at[pl.ds(SIB, ROWS)], sib_send.at[0], sib_recv.at[0], (t, g_sib))
    sib_v = remote(v_hbm, vec.at[:, pl.ds(SIB, ROWS)], sib_send.at[1], sib_recv.at[1], (t, g_sib))
    sib_y = remote(yloc.at[:, pl.ds(SIB, ROWS)], ysib, sib_send.at[2], sib_recv.at[2], (t, g_sib))

    @pl.when(light)
    def _():
        pl.semaphore_wait(barrier, 2)
        for k in range(CHUNKS):
            direct_x(k).start()
            direct_v(k).start()
            hop(k).start()

    yloc[...] = jnp.zeros_like(yloc)
    yfar[...] = jnp.zeros_like(yfar)
    kb[...] = jnp.zeros_like(kb)
    ell = ell_ref[0]
    scale = s_ref[0]
    rate = -LOG2E / jnp.full((1, STEP_C), 2.0 * (ell * ell), F32)

    def split(n):
        high = n.astype(BF16).astype(F32)
        mid = (n - high).astype(BF16).astype(F32)
        return high, mid, (n - high) - mid

    def pick(index, parts):
        out = jnp.zeros_like(parts[0])
        for i, part in enumerate(parts):
            out = jnp.where(index == i, part, out)
        return out.astype(BF16)

    def norms(off, n, with_left):
        lane = lax.broadcasted_iota(jnp.int32, (128, 128), 1)
        one = jnp.ones((128, 128), F32)
        for lo in range(0, n, 128):
            rows = pl.ds(pl.multiple_of(off + lo, 128), 128)
            x = pts[rows, :].astype(F32)
            parts = split(jnp.broadcast_to(jnp.sum(x * x, axis=1, keepdims=True), (128, 128)))
            if with_left:
                left[rows, :] = pick(lane, (*parts, one, one, one))
            right[rows, :] = pick(lane, (one, one, one, *parts))

    def all_norms(off):
        def some(i, _):
            norms(off + i * 256, 256, True)
            return 0
        lax.fori_loop(0, ROWS // 256, some, 0)

    def apply_k(k_buf, q, row, col, both):
        blk = k_buf[pl.ds(q * SUB, SUB), :]
        at = pl.ds(pl.multiple_of(row + q * SUB, SUB), SUB)
        yloc[:, at] += lax.dot_general(vec[:, pl.ds(col, STEP_C)], blk, NT, preferred_element_type=F32)
        if both:
            return jnp.dot(vec[:, at], blk, preferred_element_type=F32)
        return None

    def add_cols(col, acc, chunk):
        if chunk is None:
            yloc[:, pl.ds(col, STEP_C)] += acc
        else:
            yfar[chunk] += acc

    def columns(col):
        at = pl.ds(col, STEP_C)
        return jnp.concatenate([pts[at, :] * BF16(-2.0), right[at, :]], axis=1)

    def step(slot, row, xr, prev_row, prev_col, both, prev_chunk):
        new, old = (ka, kb) if slot == 0 else (kb, ka)
        row, subs = row
        prev_row, prev_subs = prev_row
        acc = None
        for q in range(max(subs, prev_subs)):
            if q < subs:
                at = pl.ds(pl.multiple_of(row + q * SUB, SUB), SUB)
                xl = jnp.concatenate([pts[at, :], left[at, :]], axis=1)
                dist = jnp.maximum(lax.dot_general(xl, xr, NT, preferred_element_type=F32), 0.0)
                new[pl.ds(q * SUB, SUB), :] = (scale * jnp.exp2(dist * rate)).astype(BF16)
            if q < prev_subs:
                part = apply_k(old, q, prev_row, prev_col, both)
                if both:
                    acc = part if acc is None else acc + part
        if both:
            add_cols(prev_col, acc, prev_chunk)

    def drain(row, col, both, chunk):
        row, subs = row
        acc = None
        for q in range(subs):
            part = apply_k(kb, q, row, col, both)
            if both:
                acc = part if acc is None else acc + part
        if both:
            add_cols(col, acc, chunk)

    def tile_rows(x):
        return pl.multiple_of(x, STEP_C)

    load_x.wait()
    load_v.wait()
    all_norms(OWN)

    @pl.when(heavy)
    def _():
        pl.semaphore_wait(barrier, 5)
        pl.semaphore_signal(go_sem, inc=1, device_id=(t, g_far), device_id_type=MESH)
        for k in range(LENT):
            lent_x(k).start()
            direct_v(k).start()
        sib_x.start()
        sib_v.start()

    def diag_body(i, _):
        base = i * STEP_R
        before = jnp.maximum(i - 1, 0) * STEP_R
        for q in range(4):
            if q == 0:
                prev = ((tile_rows(before), 4), tile_rows(before + 3 * STEP_C))
            else:
                prev = ((tile_rows(base), 4), tile_rows(base + (q - 1) * STEP_C))
            step(q % 2, (tile_rows(base), 4), columns(tile_rows(base + q * STEP_C)), *prev, False, None)


        @pl.when(jnp.logical_and(light, i == 1))
        def _():
            pl.semaphore_wait(go_sem, 1)
            sib_x.start()
            sib_v.start()
        return 0

    lax.fori_loop(0, 2, diag_body, 0)
    drain((STEP_R, 4), STEP_R + 3 * STEP_C, False, None)
    kb[...] = jnp.zeros_like(kb)

    def pass_on(k):
        hop(k).wait_recv()
        forward(k).start()

    @pl.when(heavy)
    def _():
        for k in PASS_OWN:
            pass_on(k)

    sib_x.wait_recv()
    sib_v.wait_recv()
    all_norms(SIB)

    def both_place(i):
        row = jnp.where(i == 0, STEP_R, core * (SIB + STEP_R))
        col = jnp.where(i == 0, 0, jnp.where(core == 0, SIB, OWN) + (i - 1) * STEP_R)
        return row, col

    def both_body(i, _):
        @pl.when(heavy)
        def _():
            for at, some in enumerate(PASS_BOTH):
                @pl.when(i == at)
                def _():
                    for k in some:
                        pass_on(k)
        row, col = both_place(i)
        row0, col0 = both_place(jnp.maximum(i - 1, 0))
        for q in range(4):
            prev = ((tile_rows(row0), 4), tile_rows(col0 + 3 * STEP_C)) if q == 0 else (
                (tile_rows(row), 4), tile_rows(col + (q - 1) * STEP_C))
            step(q % 2, (tile_rows(row), 4), columns(tile_rows(col + q * STEP_C)), *prev, True, None)
        return 0

    lax.fori_loop(0, 3, both_body, 0)
    row_end, col_end = both_place(2)
    drain((tile_rows(row_end), 4), tile_rows(col_end + 3 * STEP_C), True, None)

    def far_pass(n, order, arrive):
        if n == 0:
            return
        kb[...] = jnp.zeros_like(kb)

        def far_body(k, _):
            for j in range(n):
                @pl.when(k == j)
                def _():
                    arrive(j)
            col = tile_rows(FAR + k * STEP_C)
            norms(col, STEP_C, False)
            xr = columns(col)
            before = jnp.maximum(k - 1, 0)
            for q in range(4):
                if q == 0:
                    step(0, order[0], xr, order[3], tile_rows(FAR + before * STEP_C), True, before)
                else:
                    step(q % 2, order[q], xr, order[q - 1], col, True, k)

            @pl.when(k > 0)
            def _():
                give_back(before).start()
            return 0

        lax.fori_loop(0, n, far_body, 0)
        sib_y.start()
        drain(order[3], FAR + (n - 1) * STEP_C, True, n - 1)
        give_back(n - 1).start()

    def heavy_arrive(j):
        for k in PASS_FAR[j]:
            pass_on(k)
        direct_x(j).wait_recv()
        direct_v(j).wait_recv()
        forward(j).wait_recv()

    def light_arrive(j):
        lent_x(j).wait_recv()
        direct_v(j).wait_recv()

    def near_rows(first):
        subs = (ROWS - first) // SUB
        return [piece for base, more in ((SIB, subs - 4), (OWN, 4))
                for piece in ((base + first, more), (base + first + more * SUB, subs - more))]

    @pl.when(heavy)
    def _():
        far_pass(CHUNKS, near_rows(LENT * STEP_C), heavy_arrive)

    @pl.when(light)
    def _():
        far_pass(LENT, near_rows(0), light_arrive)

    sib_y.wait_recv()

    @pl.when(heavy)
    def _():
        for k in range(CHUNKS):
            at = pl.ds(k * STEP_C, STEP_C)
            total = yloc[:, at] + ysib[:, at]
            if k < LENT:
                give_back(k).wait_recv()
                total = total + yret[k]
            out_ref[:, at] = total
            forward(k).wait_send()
            give_back(k).wait_send()
        for k in range(LENT):
            lent_x(k).wait_send()
            direct_v(k).wait_send()

    @pl.when(light)
    def _():
        for k in range(CHUNKS):
            at = pl.ds(k * STEP_C, STEP_C)
            give_back(k).wait_recv()
            out_ref[:, at] = yloc[:, at] + ysib[:, at] + yret[k]
            direct_x(k).wait_send()
            direct_v(k).wait_send()
            hop(k).wait_send()
        for k in range(LENT):
            give_back(k).wait_send()

    sib_x.wait_send()
    sib_v.wait_send()
    sib_y.wait_send()


def solution(mesh):
    row_spec = P(('tasks', 'group'), None)
    dma = pltpu.SemaphoreType.DMA

    def local_fn(x_loc, v_loc, lengthscale, outscale):
        any_spec = pl.BlockSpec(memory_space=pl.ANY)
        smem = pl.BlockSpec(memory_space=pltpu.SMEM)
        y_t = pl.pallas_call(
            kernel,
            out_shape=jax.ShapeDtypeStruct((RHS, ROWS), F32),
            in_specs=[any_spec, any_spec, smem, smem],
            out_specs=pl.BlockSpec(memory_space=pltpu.VMEM),
            scratch_shapes=[
                pltpu.VMEM((3 * ROWS, FEATS), BF16),
                pltpu.VMEM((RHS, 3 * ROWS), BF16),
                pltpu.VMEM((2 * ROWS, 128), BF16),
                pltpu.VMEM((3 * ROWS, 128), BF16),
                pltpu.VMEM((RHS, 2 * ROWS), F32),
                pltpu.VMEM((CHUNKS, RHS, STEP_C), F32),
                pltpu.VMEM((RHS, ROWS), F32),
                pltpu.VMEM((CHUNKS, RHS, STEP_C), F32),
                pltpu.VMEM((CHUNKS, RELAY_MAX, FEATS), BF16),
                pltpu.VMEM((STEP_R, STEP_C), BF16),
                pltpu.VMEM((STEP_R, STEP_C), BF16),
                dma((2,)), pltpu.SemaphoreType.REGULAR, dma((3,)), dma((3,)),
            ] + [dma((CHUNKS,))] * 10,
            compiler_params=pltpu.CompilerParams(
                collective_id=0, has_side_effects=True, vmem_limit_bytes=40 * 2**20),
        )(pltpu.with_memory_space_constraint(x_loc, pltpu.HBM), pltpu.with_memory_space_constraint(v_loc.T, pltpu.HBM), lengthscale, outscale)
        return y_t.T

    return jax.shard_map(local_fn, mesh=mesh, in_specs=(row_spec, row_spec, P(None), P(None)), out_specs=row_spec,
                         check_vma=False)
```
